256 devices in a mesh: groups: 2 (over z), section: 64 (over y, x), head: 2 (over core).
Axes of the slice: x: 8, y: 8, z: 2, core: 2. Of those that a mesh axis runs over, the one named last changes fastest.
The devices are a block of a 8x8x16 slice.
Arguments:
- video_tokens: bfloat16 [65536, 1536], P(('groups', 'section', 'head')), parts along dimension 0, may hold values from -6 to 6
- modulation: float32 [6, 1536], P('groups'), parts along dimension 0, may hold values from -3 to 3
- project_weight: bfloat16 [3, 1536, 1536], P(None, None, 'head'), may hold values from -0.15625 to 0.15625
- output_weight: bfloat16 [1536, 1536], P('head'), may hold values from -0.15625 to 0.15625
- norm_gains: float32 [3, 128], replicated, may hold values from 1 to 2
- text_cache: bfloat16 [2, 512, 1536], P(None, 'groups', 'head'), parts along dimension 1, may hold values from -6 to 6
- text_count: int32 [2], P('groups'), parts along dimension 0, may hold values from 1 to 256, as said below
- video_keep: int32 [65536], P('groups'), parts along dimension 0, may hold values 0 or 1
- patch_order: int32 [128], P('groups'), parts along dimension 0, may hold values from 0 to 63, each once
- stale_cache: bfloat16 [2, 65536, 1536], P(None, ('groups', 'section'), 'head'), parts along dimension 1, may hold values from -6 to 6
Outputs:
- updated: bfloat16 [65536, 1536], P(('groups', 'section', 'head')), parts along dimension 0
- fresh_cache: bfloat16 [2, 65536, 1536], P(None, ('groups', 'section'), 'head'), parts along dimension 1
The draws below stay inside these ranges and needn't reach their ends.
There are 2 independent parts, one for each index of `groups`. The reference program is written for one: setup_inputs(seed, part) draws one part's arguments, and reference() takes and returns one part's arrays. A program takes and returns all parts, laid end to end along the dimension named above; an argument that names none is the same for every part. Nothing has to cross between parts.
Inputs may be any that keep to these rules, and one draw needn't show every extreme that they name: The first text_count text tokens are real, the rest are padding. `video_keep`: 1 keeps a video token as a key, 0 marks padding. `patch_order`: each place 0 to 63 is held by exactly one patch.
All inputs are finite; a program needn't handle non-finite values.
Results may differ from the reference program's by a relative error of at most 0.0049.
Values may be sent and summed in bfloat16 or wider, within the bound.
No kernel may reach another device: no remote copies, remote signals or barrier semaphores. Data moves between devices by JAX's collectives and lax.ppermute only.
A program may use at most 128 MiB of HBM per device.

```python
import jax
import jax.numpy as jnp
from jax import lax

D = 1536
HEADS = 12
HEAD_DIM = 128
TEXT = 256
PATCH = 512
HID = 1536
SEQ = 32768
N_SECTION = 64


def draw_text_count(key, part):
    short = jax.random.randint(key, (1,), 1, TEXT // 2 + 1, dtype=jnp.int32)
    odd_part = jnp.asarray(part, jnp.int32) % 2 == 1
    return jnp.where(odd_part, jnp.full((1,), TEXT, jnp.int32), short).astype(jnp.int32)


def with_ends(entries, key, low, top_value):
    extent = entries.shape
    place = [jax.random.randint(jax.random.fold_in(key, axis), (), 0, extent[axis]) for axis in range(len(extent))]
    entries = entries.at[tuple(place)].set(low)
    longest = extent.index(max(extent))
    place[longest] = (place[longest] + 1) % extent[longest]
    return entries.at[tuple(place)].set(top_value)


def block_levels(own_key, dims, cuts, least, largest):
    loudness = 1.0
    for position, blocks in cuts:
        steps = jax.random.uniform(jax.random.fold_in(jax.random.fold_in(own_key, 6), position), (blocks,), jnp.float32, least / len(cuts), largest / len(cuts))
        loudness = loudness * jnp.repeat(jnp.exp(steps), dims[position] // blocks).reshape((-1,) + (1,) * (len(dims) - 1 - position))
    return loudness


def normal_values(rng, dims, deviation, most, split=(), kind=jnp.bfloat16):
    result = deviation * jax.random.normal(rng, dims, jnp.float32)
    if split:
        result = result * block_levels(rng, dims, split, -0.22, 0.18)
    return jnp.clip(result, -most, most).astype(kind)


def setup_inputs(seed: int = 0, part: int = 0) -> dict:
    streams_of = jax.random.split(jax.random.key(seed), 11)
    own_keys = jax.random.split(jax.random.fold_in(streams_of[10], part), 11)
    video_tokens = normal_values(own_keys[0], (SEQ, D), 1.0, 6.0, ((0, 128),))
    modulation = normal_values(own_keys[1], (3, D), 0.7, 3.0, (), jnp.float32)
    project_weight = normal_values(streams_of[2], (3, D, HID), D ** -0.5, 0.15625, ((2, 2),))
    output_weight = normal_values(streams_of[3], (HID, D), HID ** -0.5, 0.15625, ((0, 2),))
    norm_gains = jnp.clip(jax.random.uniform(streams_of[4], (3, HEAD_DIM), jnp.float32, 1.0, 2.0), 1.0, 2.0)
    text_cache = normal_values(own_keys[5], (2, TEXT, HID), 1.4, 6.0, ((2, 2),))
    text_count = draw_text_count(jax.random.fold_in(jax.random.fold_in(streams_of[10], part), 71), part)
    video_keep = with_ends((jax.random.randint(own_keys[7], (SEQ,), 0, 4) < 3).astype(jnp.int32), jax.random.fold_in(own_keys[7], 1), 0, 1)
    patch_order = jax.random.permutation(own_keys[8], N_SECTION).astype(jnp.int32)
    stale_cache = normal_values(own_keys[9], (2, SEQ, HID), 1.4, 6.0, ((1, 64), (2, 2)))
    return dict(video_tokens=video_tokens, modulation=modulation, project_weight=project_weight, output_weight=output_weight, norm_gains=norm_gains, text_cache=text_cache, text_count=text_count, video_keep=video_keep, patch_order=patch_order, stale_cache=stale_cache)


epsilon = 1e-06

def widen(array):
    return lax.optimization_barrier(array).astype(jnp.float32)

def layer_norm(values):
    center = lax.optimization_barrier(jnp.mean(values, axis=-1, keepdims=True))
    shifted = values - center
    spread = lax.optimization_barrier(jnp.mean(shifted * shifted, axis=-1, keepdims=True))
    return shifted * lax.rsqrt(spread + epsilon)

def head_norm(inputs, gain_row):
    per_head = inputs.reshape(inputs.shape[0], HEADS, HEAD_DIM)
    scaled = per_head * lax.rsqrt(lax.optimization_barrier(jnp.mean(per_head * per_head, axis=-1, keepdims=True)) + epsilon) * gain_row
    return scaled.astype(jnp.bfloat16)

def reference(video_tokens, modulation, project_weight, output_weight, norm_gains, text_cache, text_count, video_keep, patch_order, stale_cache):
    hidden = video_tokens.astype(jnp.float32)
    normed = (layer_norm(hidden) * (1.0 + modulation[1]) + modulation[0]).astype(jnp.bfloat16)
    projected = jnp.einsum('sd,cdh->csh', widen(normed), project_weight.astype(jnp.float32), precision=lax.Precision.HIGHEST)
    fresh_cache = projected[1:3].astype(jnp.bfloat16)
    queries = head_norm(projected[0], norm_gains[0])
    fresh_keys = head_norm(widen(fresh_cache[0]), norm_gains[1])
    stale_keys = head_norm(stale_cache[0].astype(jnp.float32), norm_gains[1])
    text_keys = head_norm(text_cache[0].astype(jnp.float32), norm_gains[2])
    fresh_values = fresh_cache[1].reshape(SEQ, HEADS, HEAD_DIM)
    stale_values = stale_cache[1].reshape(SEQ, HEADS, HEAD_DIM)
    text_values = text_cache[1].reshape(TEXT, HEADS, HEAD_DIM)
    text_live = jnp.arange(TEXT, dtype=jnp.int32) < text_count[0]
    score_scale = HEAD_DIM ** (-0.5)

    def rows_of(array, patch_index):
        return lax.dynamic_slice_in_dim(array, (patch_index * PATCH).astype(jnp.int32), PATCH, 0)

    def one_patch(patch_index):
        left_place = jnp.maximum(patch_index - 1, 0).astype(jnp.int32)
        right_place = jnp.minimum(patch_index + 1, N_SECTION - 1).astype(jnp.int32)
        own_slot = patch_order[patch_index]
        left_fresh = patch_order[left_place] < own_slot
        right_fresh = patch_order[right_place] < own_slot
        left_keys = jnp.where(left_fresh, rows_of(fresh_keys, left_place), rows_of(stale_keys, left_place))
        right_keys = jnp.where(right_fresh, rows_of(fresh_keys, right_place), rows_of(stale_keys, right_place))
        left_values = jnp.where(left_fresh, rows_of(fresh_values, left_place), rows_of(stale_values, left_place))
        right_values = jnp.where(right_fresh, rows_of(fresh_values, right_place), rows_of(stale_values, right_place))
        key_rows = jnp.concatenate([left_keys, rows_of(fresh_keys, patch_index), right_keys, text_keys], axis=0)
        value_rows = jnp.concatenate([left_values, rows_of(fresh_values, patch_index), right_values, text_values], axis=0)
        key_live = jnp.concatenate([(rows_of(video_keep, left_place) > 0) & (patch_index > 0), rows_of(video_keep, patch_index) > 0, (rows_of(video_keep, right_place) > 0) & (patch_index < N_SECTION - 1), text_live])
        query_rows = rows_of(queries, patch_index)
        scores = jnp.einsum('qhd,khd->hqk', query_rows.astype(jnp.float32), key_rows.astype(jnp.float32), precision=lax.Precision.HIGHEST) * score_scale
        weights = jnp.where(key_live[None, None, :], jnp.exp(scores), 0.0)
        total = lax.optimization_barrier(jnp.sum(weights, axis=-1))
        numerator = jnp.einsum('hqk,khd->qhd', widen(weights.astype(jnp.bfloat16)), value_rows.astype(jnp.float32), precision=lax.Precision.HIGHEST)
        return (numerator / jnp.transpose(total)[:, :, None]).astype(jnp.bfloat16).reshape(PATCH, HID)
    attended = lax.map(one_patch, jnp.arange(N_SECTION, dtype=jnp.int32)).reshape(SEQ, HID)
    mixed = jnp.dot(attended, output_weight, preferred_element_type=jnp.float32)
    updated = (hidden + modulation[2] * mixed).astype(jnp.bfloat16)
    return (updated, fresh_cache)
```

```python
import functools
import math

import jax
import jax.numpy as jnp
from jax import lax
from jax.experimental import pallas as pl
from jax.experimental.pallas import tpu as pltpu
from jax.sharding import PartitionSpec as P


epsilon = 1e-06
f32 = jnp.float32
bf16 = jnp.bfloat16
MIB = 1024 * 1024

VMEM = pl.BlockSpec(memory_space=pltpu.VMEM)
SMEM = pl.BlockSpec(memory_space=pltpu.SMEM)
HBM = pl.BlockSpec(memory_space=pltpu.HBM)


def params(mib):
    return pltpu.CompilerParams(vmem_limit_bytes=mib * MIB)


def in_hbm(array):
    return pltpu.with_memory_space_constraint(array, pltpu.HBM)


def cost(flops, nbytes):
    return pl.CostEstimate(flops=flops, bytes_accessed=nbytes, transcendentals=0)


def slots(place, order, sections):
    p = place[0]
    left = jnp.maximum(p - 1, 0)
    right = jnp.minimum(p + 1, sections - 1)
    return order[p], order[left], order[right]


def gain_row(gains, which):
    return gains[which : which + 1, :]


def head_normed(part, gain):
    spread = jnp.mean(part * part, axis=-1, keepdims=True)
    return (part * lax.rsqrt(spread + epsilon) * gain).astype(bf16)


def heads_normed(part, gain):
    size = gain.shape[-1]
    pieces = [
        head_normed(part[:, i : i + size], gain) for i in range(0, part.shape[-1], size)
    ]
    return jnp.concatenate(pieces, axis=-1)


def mask_columns(row, lanes):
    return jnp.broadcast_to(row, (lanes, row.shape[1])).T.astype(bf16)


def first_kernel(sections, place, order, x, mod, stale, normed, to_right, to_left, held, sem):
    load = pltpu.make_async_copy(stale.at[0], held, sem)
    load.start()
    rows, width = x.shape
    step = 64
    scale = 1.0 + mod[1:2, :]
    shift = mod[0:1, :]
    for r in range(0, rows, step):
        v = x[r : r + step, :].astype(f32)
        shifted = v - jnp.mean(v, axis=-1, keepdims=True)
        spread = jnp.mean(shifted * shifted, axis=-1, keepdims=True)
        normed[r : r + step, :] = (shifted * lax.rsqrt(spread + epsilon) * scale + shift).astype(
            bf16
        )
    load.wait()
    own, left, right = slots(place, order, sections)
    half = width // 2

    def fill(out, fresh):
        @pl.when(fresh)
        def _():
            out[...] = normed[...]

        @pl.when(jnp.logical_not(fresh))
        def _():
            out[:, :half] = held[:rows, :]
            out[:, half:] = held[rows:, :]

    fill(to_right, own < right)
    fill(to_left, own < left)


def project_kernel(
    sections,
    place,
    side,
    order,
    own_half,
    other_half,
    weight,
    gains,
    stale,
    cache,
    queries,
    keys,
    to_right,
    to_left,
    wbuf,
    held,
    wsem,
    sem,
):
    rows = own_half.shape[0]
    width = queries.shape[1]
    block = wbuf.shape[2]
    blocks = width // block
    size = gains.shape[1]
    kinds = (2, 1, 0)
    copies = []
    for t, c in enumerate(kinds):
        for j in range(blocks):
            n = t * blocks + j
            copy = pltpu.make_async_copy(
                weight.at[c, :, j * block : (j + 1) * block], wbuf.at[n], wsem.at[n]
            )
            copy.start()
            copies.append(copy)
    load = pltpu.make_async_copy(stale.at[1], held, sem)
    load.start()
    h = side[0]
    places = (
        (own_half, pl.multiple_of(h * rows, rows)),
        (other_half, pl.multiple_of((1 - h) * rows, rows)),
    )
    factor = math.log2(math.e) * size**-0.5
    query_gain = gain_row(gains, 0) * factor
    key_gain = gain_row(gains, 1)
    for t, c in enumerate(kinds):
        for j in range(blocks):
            n = t * blocks + j
            copies[n].wait()
            cols = slice(j * block, (j + 1) * block)
            for half, at in places:
                y = jnp.dot(half[...], wbuf[n], preferred_element_type=f32)
                at = pl.ds(at, rows)
                if c == 0:
                    queries[at, cols] = heads_normed(y, query_gain)
                else:
                    rounded = y.astype(bf16)
                    cache[c - 1, at, cols] = rounded
                    if c == 1:
                        keys[at, cols] = heads_normed(rounded.astype(f32), key_gain)
        if c == 2:
            load.wait()
            own, left, right = slots(place, order, sections)
            for out, fresh in ((to_right, own < right), (to_left, own < left)):

                @pl.when(fresh)
                def _():
                    out[...] = cache[1]

                @pl.when(jnp.logical_not(fresh))
                def _():
                    out[...] = held[...]


def own_kernel(place, count, queries, keys, cache, text, gains, keep, total, vbuf):
    patch, width = queries.shape
    text_rows = text.shape[1]
    size = gains.shape[1]
    own_mask = mask_columns((keep[pl.ds(place[0], 1), :] > 0).astype(f32), size)
    live = lax.broadcasted_iota(jnp.int32, (text_rows, size), 0) < count[0]
    text_mask = live.astype(f32).astype(bf16)
    vbuf[:patch, size:] = own_mask
    vbuf[patch:, size:] = text_mask
    gain = gain_row(gains, 2)
    for h in range(width // size):
        cols = slice(h * size, (h + 1) * size)
        text_key = head_normed(text[0, :, cols].astype(f32), gain)
        all_keys = jnp.concatenate([keys[:, cols], text_key], axis=0)
        vbuf[:patch, :size] = cache[1, :, cols] * own_mask
        vbuf[patch:, :size] = text[1, :, cols] * text_mask
        s = lax.dot_general(
            queries[:, cols], all_keys, (((1,), (1,)), ((), ())), preferred_element_type=f32
        )
        w = jnp.exp2(s).astype(bf16)
        total[:, 2 * h * size : 2 * (h + 1) * size] = jnp.dot(
            w, vbuf[...], preferred_element_type=f32
        )


def near_kernel(
    sections,
    place,
    side,
    order,
    left_own,
    left_other,
    right_own,
    right_other,
    weight,
    gains,
    queries,
    weights,
    wbuf,
    kbuf,
    wsem,
):
    rows = left_own.shape[0]
    patch, width = queries.shape
    block = wbuf.shape[2]
    size = gains.shape[1]
    copies = []
    for j in range(width // block):
        copy = pltpu.make_async_copy(
            weight.at[1, :, j * block : (j + 1) * block], wbuf.at[j], wsem.at[j]
        )
        copy.start()
        copies.append(copy)
    h = side[0]
    own_at = pl.multiple_of(h * rows, rows)
    other_at = pl.multiple_of((1 - h) * rows, rows)
    own, left, right = slots(place, order, sections)
    gain = gain_row(gains, 1)
    for j in range(width // block):
        copies[j].wait()
        for n, (mine, other, fresh) in enumerate(
            ((left_own, left_other, left < own), (right_own, right_other, right < own))
        ):
            base = n * patch

            @pl.when(fresh)
            def _():
                for half, at in ((mine, own_at), (other, other_at)):
                    y = jnp.dot(half[...], wbuf[j], preferred_element_type=f32).astype(bf16)
                    kbuf[pl.ds(base + at, rows), :] = heads_normed(y.astype(f32), gain)

            @pl.when(jnp.logical_not(fresh))
            def _():
                for i in range(patch // rows):
                    y = mine[:, i * width + j * block : i * width + (j + 1) * block]
                    kbuf[base + i * rows : base + (i + 1) * rows, :] = heads_normed(
                        y.astype(f32), gain
                    )

        for i in range(block // size):
            cols = slice(j * block + i * size, j * block + (i + 1) * size)
            s = lax.dot_general(
                queries[:, cols],
                kbuf[:, i * size : (i + 1) * size],
                (((1,), (1,)), ((), ())),
                preferred_element_type=f32,
            )
            weights[j * (block // size) + i] = jnp.exp2(s).astype(bf16)


def last_kernel(
    sections, flip, place, side, weights, left_values, right_values, total, keep, weight, out,
    vbuf, att, wbuf, wsem,
):
    load = pltpu.make_async_copy(weight, wbuf, wsem)
    load.start()
    rows = out.shape[0]
    heads, patch, _ = weights.shape
    size = vbuf.shape[1] // 2
    p = place[0]
    h = side[0]
    at = pl.ds(pl.multiple_of((1 - h if flip else h) * rows, rows), rows)
    left_row = keep[pl.ds(jnp.maximum(p - 1, 0), 1), :]
    right_row = keep[pl.ds(jnp.minimum(p + 1, sections - 1), 1), :]
    left_mask = mask_columns(((left_row > 0) & (p > 0)).astype(f32), size)
    right_mask = mask_columns(((right_row > 0) & (p < sections - 1)).astype(f32), size)
    vbuf[:patch, size:] = left_mask
    vbuf[patch:, size:] = right_mask
    for i in range(heads):
        cols = slice(i * size, (i + 1) * size)
        vbuf[:patch, :size] = left_values[:, cols] * left_mask
        vbuf[patch:, :size] = right_values[:, cols] * right_mask
        sums = total[at, 2 * i * size : 2 * (i + 1) * size] + jnp.dot(
            weights[i, at, :], vbuf[...], preferred_element_type=f32
        )
        att[:, cols] = (sums[:, :size] / sums[:, size:]).astype(bf16)
    load.wait()
    out[...] = jnp.dot(att[...], wbuf[...], preferred_element_type=f32).astype(bf16)


def swapped(array):
    return lax.ppermute(array, "head", [(0, 1), (1, 0)])


def from_behind(array, axis, by):
    count = lax.axis_size(axis)
    pairs = [(i, i + by) for i in range(count) if 0 <= i + by < count]
    return lax.ppermute(array, axis, pairs)


def on_device(
    video_tokens,
    modulation,
    project_weight,
    output_weight,
    norm_gains,
    text_cache,
    text_count,
    video_keep,
    patch_order,
    stale_cache,
):
    sections = lax.axis_size("section")
    place = lax.axis_index("section").astype(jnp.int32).reshape(1)
    side = lax.axis_index("head").astype(jnp.int32).reshape(1)
    rows, model = video_tokens.shape
    size = norm_gains.shape[1]
    width = project_weight.shape[2]
    heads = width // size
    patch = stale_cache.shape[1]
    text_rows = text_cache.shape[1]
    block = 2 * size
    project_weight = in_hbm(project_weight)
    output_weight = in_hbm(output_weight)
    stale_cache = in_hbm(stale_cache)
    keep = video_keep.reshape(sections, patch)
    half_shape = jax.ShapeDtypeStruct((rows, model), bf16)
    side_shape = jax.ShapeDtypeStruct((patch, width), bf16)

    normed, to_right, to_left = pl.pallas_call(
        functools.partial(first_kernel, sections),
        out_shape=(half_shape, half_shape, half_shape),
        in_specs=[SMEM, SMEM, VMEM, VMEM, HBM],
        out_specs=(VMEM, VMEM, VMEM),
        scratch_shapes=[pltpu.VMEM((patch, width), bf16), pltpu.SemaphoreType.DMA],
        compiler_params=params(10),
        cost_estimate=cost(10 * rows * model, 10 * rows * model),
        name="first",
    )(place, patch_order, video_tokens, modulation, stale_cache)

    other = swapped(normed)
    left_own = from_behind(to_right, "section", 1)
    right_own = from_behind(to_left, "section", -1)

    fresh_cache, queries, keys, values_right, values_left = pl.pallas_call(
        functools.partial(project_kernel, sections),
        out_shape=(
            jax.ShapeDtypeStruct((2, patch, width), bf16),
            side_shape,
            side_shape,
            side_shape,
            side_shape,
        ),
        in_specs=[SMEM, SMEM, SMEM, VMEM, VMEM, HBM, VMEM, HBM],
        out_specs=(VMEM,) * 5,
        scratch_shapes=[
            pltpu.VMEM((3 * width // block, model, block), bf16),
            pltpu.VMEM((patch, width), bf16),
            pltpu.SemaphoreType.DMA((3 * width // block,)),
            pltpu.SemaphoreType.DMA,
        ],
        compiler_params=params(24),
        cost_estimate=cost(2 * patch * model * 3 * width, 6 * model * width),
        name="project",
    )(place, side, patch_order, normed, other, project_weight, norm_gains, stale_cache)

    left_values = from_behind(values_right, "section", 1)
    right_values = from_behind(values_left, "section", -1)
    left_own, right_own, queries = lax.optimization_barrier((left_own, right_own, queries))
    left_other = swapped(left_own)
    right_other = swapped(right_own)

    total = pl.pallas_call(
        own_kernel,
        out_shape=jax.ShapeDtypeStruct((patch, 2 * width), f32),
        in_specs=[SMEM, SMEM] + [VMEM] * 6,
        out_specs=VMEM,
        scratch_shapes=[pltpu.VMEM((patch + text_rows, 2 * size), bf16)],
        compiler_params=params(20),
        cost_estimate=cost(8 * patch * (patch + text_rows) * width, 6 * patch * width),
        name="own",
    )(place, text_count, queries, keys, fresh_cache, text_cache, norm_gains, keep)

    weights = pl.pallas_call(
        functools.partial(near_kernel, sections),
        out_shape=jax.ShapeDtypeStruct((heads, patch, 2 * patch), bf16),
        in_specs=[SMEM] * 3 + [VMEM] * 4 + [HBM, VMEM, VMEM],
        out_specs=VMEM,
        scratch_shapes=[
            pltpu.VMEM((width // block, model, block), bf16),
            pltpu.VMEM((2 * patch, block), bf16),
            pltpu.SemaphoreType.DMA((width // block,)),
        ],
        compiler_params=params(24),
        cost_estimate=cost(4 * patch * model * width + 8 * patch * patch * width, 6 * patch * width),
        name="near",
    )(
        place,
        side,
        patch_order,
        left_own,
        left_other,
        right_own,
        right_other,
        project_weight,
        norm_gains,
        queries,
    )

    def finish(flip):
        return pl.pallas_call(
            functools.partial(last_kernel, sections, flip),
            out_shape=half_shape,
            in_specs=[SMEM, SMEM] + [VMEM] * 5 + [HBM],
            out_specs=VMEM,
            scratch_shapes=[
                pltpu.VMEM((2 * patch, 2 * size), bf16),
                pltpu.VMEM((rows, width), bf16),
                pltpu.VMEM((width, model), bf16),
                pltpu.SemaphoreType.DMA,
            ],
            compiler_params=params(26),
            cost_estimate=cost(
                8 * rows * patch * width + 2 * rows * width * model, 6 * patch * width
            ),
            name="last_sent" if flip else "last_kept",
        )(place, side, weights, left_values, right_values, total, keep, output_weight)

    sent = finish(True)
    received = swapped(sent)
    kept = finish(False)
    mixed = kept.astype(f32) + received.astype(f32)
    updated = (video_tokens.astype(f32) + modulation[2] * mixed).astype(bf16)
    return (updated, fresh_cache)


def solution(mesh):
    placed = (
        P(("groups", "section", "head"), None),
        P("groups", None),
        P(None, None, "head"),
        P("head", None),
        P(),
        P(None, "groups", "head"),
        P("groups"),
        P("groups"),
        P("groups"),
        P(None, ("groups", "section"), "head"),
    )

    return jax.shard_map(
        on_device,
        mesh=mesh,
        in_specs=placed,
        out_specs=(P(("groups", "section", "head"), None), P(None, ("groups", "section"), "head")),
        check_vma=False,
    )
```

```python
import functools
import math

import jax
import jax.numpy as jnp
from jax import lax
from jax.experimental import pallas as pl
from jax.experimental.pallas import tpu as pltpu
from jax.sharding import PartitionSpec as P


epsilon = 1e-06
f32 = jnp.float32
bf16 = jnp.bfloat16
MIB = 1024 * 1024

VMEM = pl.BlockSpec(memory_space=pltpu.VMEM)
SMEM = pl.BlockSpec(memory_space=pltpu.SMEM)
HBM = pl.BlockSpec(memory_space=pltpu.HBM)


def params(mib):
    return pltpu.CompilerParams(vmem_limit_bytes=mib * MIB)


def in_hbm(array):
    return pltpu.with_memory_space_constraint(array, pltpu.HBM)


def cost(flops, nbytes):
    return pl.CostEstimate(flops=flops, bytes_accessed=nbytes, transcendentals=0)


def slots(place, order, sections):
    p = place[0]
    left = jnp.maximum(p - 1, 0)
    right = jnp.minimum(p + 1, sections - 1)
    return order[p], order[left], order[right]


def gain_row(gains, which):
    return gains[which : which + 1, :]


def head_normed(part, gain):
    spread = jnp.mean(part * part, axis=-1, keepdims=True)
    return (part * lax.rsqrt(spread + epsilon) * gain).astype(bf16)


def heads_normed(part, gain):
    size = gain.shape[-1]
    pieces = [
        head_normed(part[:, i : i + size], gain) for i in range(0, part.shape[-1], size)
    ]
    return jnp.concatenate(pieces, axis=-1)


def mask_columns(row, lanes):
    return jnp.broadcast_to(row, (lanes, row.shape[1])).T.astype(bf16)


def first_kernel(
    sections, place, order_in, x_in, mod_in, stale, normed, to_right, to_left, values,
    order, x, mod, held, sems,
):
    copies = [
        pltpu.make_async_copy(source, target, sems.at[i])
        for i, (source, target) in enumerate(
            (
                (order_in, order),
                (x_in, x),
                (mod_in, mod),
                (stale.at[0], held),
                (stale.at[1], values),
            )
        )
    ]
    for copy in copies:
        copy.start()
    rows, width = x.shape
    for copy in copies[:3]:
        copy.wait()
    scale = 1.0 + mod[1:2, :]
    shift = mod[0:1, :]
    step = 64
    for r in range(0, rows, step):
        v = x[r : r + step, :].astype(f32)
        shifted = v - jnp.mean(v, axis=-1, keepdims=True)
        spread = jnp.mean(shifted * shifted, axis=-1, keepdims=True)
        normed[r : r + step, :] = (shifted * lax.rsqrt(spread + epsilon) * scale + shift).astype(
            bf16
        )
    copies[3].wait()
    own, left, right = slots(place, order, sections)
    half = width // 2

    def fill(out, fresh):
        @pl.when(fresh)
        def _():
            out[...] = normed[...]

        @pl.when(jnp.logical_not(fresh))
        def _():
            out[:, :half] = held[:rows, :]
            out[:, half:] = held[rows:, :]

    fill(to_right, own < right)
    fill(to_left, own < left)
    copies[4].wait()


def attend(queries, keys, vbuf):
    s = lax.dot_general(queries, keys, (((1,), (1,)), ((), ())), preferred_element_type=f32)
    return jnp.dot(jnp.exp2(s).astype(bf16), vbuf, preferred_element_type=f32)


def project_kernel(
    place,
    side,
    count,
    own_half,
    other_half,
    weight,
    gains,
    text,
    keep,
    cache,
    queries,
    total,
    key_weight,
    value_weight,
    query_weight,
    keys,
    vbuf,
    sems,
):
    rows = own_half.shape[0]
    patch, width = queries.shape
    text_rows = text.shape[1]
    size = gains.shape[1]
    block = 2 * size
    buffers = {2: value_weight, 1: key_weight, 0: query_weight}
    pieces = ((2, 0, block), (2, block, width), (1, 0, width), (0, 0, width))
    copies = []
    for n, (c, low, high) in enumerate(pieces):
        copy = pltpu.make_async_copy(
            weight.at[c, :, low:high], buffers[c].at[:, low:high], sems.at[n]
        )
        copy.start()
        copies.append(copy)
    own_mask = mask_columns((keep[pl.ds(place[0], 1), :] > 0).astype(f32), size)
    live = lax.broadcasted_iota(jnp.int32, (text_rows, size), 0) < count[0]
    text_mask = live.astype(f32).astype(bf16)
    heads = width // size
    text_gain = gain_row(gains, 2)
    for i in range(heads):
        cols = slice(i * size, (i + 1) * size)
        keys[patch:, cols] = head_normed(text[0, :, cols].astype(f32), text_gain)
        vbuf[i, :patch, size:] = own_mask
        vbuf[i, patch:, size:] = text_mask
        vbuf[i, patch:, :size] = text[1, :, cols] * text_mask
    h = side[0]
    places = (
        (own_half, pl.multiple_of(h * rows, rows)),
        (other_half, pl.multiple_of((1 - h) * rows, rows)),
    )
    factor = math.log2(math.e) * size**-0.5
    query_gain = gain_row(gains, 0) * factor
    key_gain = gain_row(gains, 1)
    for n, (c, low, high) in enumerate(pieces):
        copies[n].wait()
        for j in range(low, high, block):
            cols = slice(j, j + block)
            for half, at in places:
                y = jnp.dot(half[...], buffers[c][:, cols], preferred_element_type=f32)
                at = pl.ds(at, rows)
                if c == 0:
                    queries[at, cols] = heads_normed(y, query_gain)
                else:
                    rounded = y.astype(bf16)
                    cache[c - 1, at, cols] = rounded
                    if c == 1:
                        keys[at, cols] = heads_normed(rounded.astype(f32), key_gain)
    for i in range(heads):
        cols = slice(i * size, (i + 1) * size)
        vbuf[i, :patch, :size] = cache[1, :, cols] * own_mask
        total[:, 2 * i * size : 2 * (i + 1) * size] = attend(
            queries[:, cols], keys[:, cols], vbuf[i]
        )


def side_mask(keep, place, sections, by, size):
    wanted = place[0] + by
    there = (wanted >= 0) & (wanted < sections)
    row = keep[pl.ds(jnp.clip(wanted, 0, sections - 1), 1), :]
    return mask_columns(((row > 0) & there).astype(f32), size)


def add_side(queries, keys, vbuf, total, size):
    for i in range(queries.shape[1] // size):
        cols = slice(i * size, (i + 1) * size)
        wide = slice(2 * i * size, 2 * (i + 1) * size)
        total[:, wide] += attend(queries[:, cols], keys[:, cols], vbuf[i])


def fresh_kernel(
    sections,
    place,
    side,
    order,
    left_own,
    left_other,
    right_own,
    right_other,
    key_weight,
    value_weight,
    gains,
    queries,
    keep,
    total_in,
    total,
    keys,
    vbuf,
):
    rows = left_own.shape[0]
    _, width = queries.shape
    size = gains.shape[1]
    block = 2 * size
    h = side[0]
    own, left, right = slots(place, order, sections)
    gain = gain_row(gains, 1)
    total[...] = total_in[...]
    for mine, other, fresh, by in (
        (left_own, left_other, left < own, -1),
        (right_own, right_other, right < own, 1),
    ):

        @pl.when(fresh)
        def _():
            mask = side_mask(keep, place, sections, by, size)
            for i in range(width // size):
                vbuf[i, :, size:] = mask
            for half, at in ((mine, h), (other, 1 - h)):
                at = pl.ds(pl.multiple_of(at * rows, rows), rows)
                for j in range(0, width, block):
                    cols = slice(j, j + block)
                    y = jnp.dot(half[...], key_weight[:, cols], preferred_element_type=f32)
                    keys[at, cols] = heads_normed(y.astype(bf16).astype(f32), gain)
                for j in range(0, width, block):
                    cols = slice(j, j + block)
                    y = jnp.dot(half[...], value_weight[:, cols], preferred_element_type=f32)
                    y = y.astype(bf16)
                    for i in range(block // size):
                        vbuf[j // size + i, at, :size] = (
                            y[:, i * size : (i + 1) * size] * vbuf[0, at, size:]
                        )
            add_side(queries, keys, vbuf, total, size)


def stale_kernel(
    sections,
    place,
    side,
    order,
    left_keys,
    left_values,
    right_keys,
    right_values,
    gains,
    queries,
    keep,
    total_in,
    weight,
    sent,
    kept,
    keys,
    vbuf,
    total,
    att,
):
    rows = sent.shape[0]
    patch, width = queries.shape
    size = gains.shape[1]
    p = place[0]
    h = side[0]
    own, left, right = slots(place, order, sections)
    gain = gain_row(gains, 1)
    total[...] = total_in[...]
    for raw, values, wanted, by in (
        (left_keys, left_values, (left > own) & (p > 0), -1),
        (right_keys, right_values, (right > own) & (p < sections - 1), 1),
    ):

        @pl.when(wanted)
        def _():
            mask = side_mask(keep, place, sections, by, size)
            for r in range(patch // rows):
                keys[r * rows : (r + 1) * rows, :] = heads_normed(
                    raw[:, r * width : (r + 1) * width].astype(f32), gain
                )
            for i in range(width // size):
                cols = slice(i * size, (i + 1) * size)
                vbuf[i, :, size:] = mask
                vbuf[i, :, :size] = values[:, cols] * mask
            add_side(queries, keys, vbuf, total, size)

    for i in range(width // size):
        low = 2 * i * size
        att[:, i * size : (i + 1) * size] = (
            total[:, low : low + size] / total[:, low + size : low + 2 * size]
        ).astype(bf16)
    for out, at in ((sent, 1 - h), (kept, h)):
        at = pl.ds(pl.multiple_of(at * rows, rows), rows)
        out[...] = jnp.dot(att[at, :], weight[...], preferred_element_type=f32).astype(bf16)


def swapped(array):
    return lax.ppermute(array, "head", [(0, 1), (1, 0)])


def from_behind(array, axis, by):
    count = lax.axis_size(axis)
    pairs = [(i, i + by) for i in range(count) if 0 <= i + by < count]
    return lax.ppermute(array, axis, pairs)


def on_device(
    video_tokens,
    modulation,
    project_weight,
    output_weight,
    norm_gains,
    text_cache,
    text_count,
    video_keep,
    patch_order,
    stale_cache,
):
    sections = lax.axis_size("section")
    place = lax.axis_index("section").astype(jnp.int32).reshape(1)
    side = lax.axis_index("head").astype(jnp.int32).reshape(1)
    rows, model = video_tokens.shape
    size = norm_gains.shape[1]
    width = project_weight.shape[2]
    heads = width // size
    patch = stale_cache.shape[1]
    text_rows = text_cache.shape[1]
    keep = video_keep.reshape(sections, patch)
    half_shape = jax.ShapeDtypeStruct((rows, model), bf16)
    side_shape = jax.ShapeDtypeStruct((patch, width), bf16)
    weight_shape = jax.ShapeDtypeStruct((model, width), bf16)
    total_shape = jax.ShapeDtypeStruct((patch, 2 * width), f32)

    normed, to_right, to_left, values = pl.pallas_call(
        functools.partial(first_kernel, sections),
        out_shape=(half_shape, half_shape, half_shape, side_shape),
        in_specs=[SMEM, HBM, HBM, HBM, HBM],
        out_specs=(VMEM,) * 4,
        scratch_shapes=[
            pltpu.SMEM(patch_order.shape, jnp.int32),
            pltpu.VMEM((rows, model), bf16),
            pltpu.VMEM(modulation.shape, f32),
            pltpu.VMEM((patch, width), bf16),
            pltpu.SemaphoreType.DMA((5,)),
        ],
        compiler_params=params(10),
        cost_estimate=cost(10 * rows * model, 10 * rows * model),
        name="first",
    )(
        place,
        in_hbm(patch_order),
        in_hbm(video_tokens),
        in_hbm(modulation),
        in_hbm(stale_cache),
    )

    left_own = from_behind(to_right, "section", 1)
    right_own = from_behind(to_left, "section", -1)
    left_values = from_behind(values, "section", 1)
    right_values = from_behind(values, "section", -1)
    other = swapped(normed)

    fresh_cache, queries, total, key_weight, value_weight = pl.pallas_call(
        project_kernel,
        out_shape=(
            jax.ShapeDtypeStruct((2, patch, width), bf16),
            side_shape,
            total_shape,
            weight_shape,
            weight_shape,
        ),
        in_specs=[SMEM, SMEM, SMEM, VMEM, VMEM, HBM, VMEM, VMEM, VMEM],
        out_specs=(VMEM,) * 5,
        scratch_shapes=[
            pltpu.VMEM((model, width), bf16),
            pltpu.VMEM((patch + text_rows, width), bf16),
            pltpu.VMEM((heads, patch + text_rows, 2 * size), bf16),
            pltpu.SemaphoreType.DMA((4,)),
        ],
        compiler_params=params(28),
        cost_estimate=cost(2 * patch * model * 3 * width, 6 * model * width),
        name="project",
    )(
        place,
        side,
        text_count,
        normed,
        other,
        in_hbm(project_weight),
        norm_gains,
        text_cache,
        keep,
    )

    left_own, right_own, queries = lax.optimization_barrier((left_own, right_own, queries))
    left_other = swapped(left_own)
    right_other = swapped(right_own)

    total = pl.pallas_call(
        functools.partial(fresh_kernel, sections),
        out_shape=total_shape,
        in_specs=[SMEM] * 3 + [VMEM] * 10,
        out_specs=VMEM,
        scratch_shapes=[
            pltpu.VMEM((patch, width), bf16),
            pltpu.VMEM((heads, patch, 2 * size), bf16),
        ],
        input_output_aliases={12: 0},
        compiler_params=params(24),
        cost_estimate=cost(4 * patch * model * width, 6 * patch * width),
        name="fresh",
    )(
        place,
        side,
        patch_order,
        left_own,
        left_other,
        right_own,
        right_other,
        key_weight,
        value_weight,
        norm_gains,
        queries,
        keep,
        total,
    )

    sent, kept = pl.pallas_call(
        functools.partial(stale_kernel, sections),
        out_shape=(half_shape, half_shape),
        in_specs=[SMEM] * 3 + [VMEM] * 9,
        out_specs=(VMEM, VMEM),
        scratch_shapes=[
            pltpu.VMEM((patch, width), bf16),
            pltpu.VMEM((heads, patch, 2 * size), bf16),
            pltpu.VMEM((patch, 2 * width), f32),
            pltpu.VMEM((patch, width), bf16),
        ],
        compiler_params=params(24),
        cost_estimate=cost(2 * patch * width * model, 6 * patch * width),
        name="stale",
    )(
        place,
        side,
        patch_order,
        left_own,
        left_values,
        right_own,
        right_values,
        norm_gains,
        queries,
        keep,
        total,
        output_weight,
    )
    received = swapped(sent)
    mixed = kept.astype(f32) + received.astype(f32)
    updated = (video_tokens.astype(f32) + modulation[2] * mixed).astype(bf16)
    return (updated, fresh_cache)


def solution(mesh):
    placed = (
        P(("groups", "section", "head"), None),
        P("groups", None),
        P(None, None, "head"),
        P("head", None),
        P(),
        P(None, "groups", "head"),
        P("groups"),
        P("groups"),
        P("groups"),
        P(None, ("groups", "section"), "head"),
    )

    return jax.shard_map(
        on_device,
        mesh=mesh,
        in_specs=placed,
        out_specs=(P(("groups", "section", "head"), None), P(None, ("groups", "section"), "head")),
        check_vma=False,
    )
```

```python
import functools
import math

import jax
import jax.numpy as jnp
from jax import lax
from jax.experimental import pallas as pl
from jax.experimental.pallas import tpu as pltpu
from jax.sharding import PartitionSpec as P


epsilon = 1e-06
f32 = jnp.float32
bf16 = jnp.bfloat16
MIB = 1024 * 1024

VMEM = pl.BlockSpec(memory_space=pltpu.VMEM)
SMEM = pl.BlockSpec(memory_space=pltpu.SMEM)
HBM = pl.BlockSpec(memory_space=pltpu.HBM)


def params(mib):
    return pltpu.CompilerParams(vmem_limit_bytes=mib * MIB)


def in_hbm(array):
    return pltpu.with_memory_space_constraint(array, pltpu.HBM)


def cost(flops, nbytes):
    return pl.CostEstimate(flops=flops, bytes_accessed=nbytes, transcendentals=0)


def slots(place, order, sections):
    p = place[0]
    left = jnp.maximum(p - 1, 0)
    right = jnp.minimum(p + 1, sections - 1)
    return order[p], order[left], order[right]


def gain_row(gains, which):
    return gains[which : which + 1, :]


def head_normed(part, gain):
    spread = jnp.mean(part * part, axis=-1, keepdims=True)
    return (part * lax.rsqrt(spread + epsilon) * gain).astype(bf16)


def heads_normed(part, gain):
    size = gain.shape[-1]
    pieces = [
        head_normed(part[:, i : i + size], gain) for i in range(0, part.shape[-1], size)
    ]
    return jnp.concatenate(pieces, axis=-1)


def mask_columns(row, lanes):
    return jnp.broadcast_to(row, (lanes, row.shape[1])).T.astype(bf16)


def first_kernel(
    sections, place, order_in, x_in, mod_in, stale, normed_out, to_right, to_left, values_out,
    order, x, mod, held, values, normed, sems, out_sems,
):
    rows, width = x.shape
    part = rows // 2
    half = width // 2
    loads = [(mod_in, mod)] + [(x_in.at[r : r + part], x.at[r : r + part]) for r in (0, part)]
    loads += [(order_in, order), (stale.at[0], held), (stale.at[1], values)]
    copies = [
        pltpu.make_async_copy(source, target, sems.at[i])
        for i, (source, target) in enumerate(loads)
    ]
    for copy in copies:
        copy.start()
    copies[0].wait()
    scale = 1.0 + mod[1:2, :]
    shift = mod[0:1, :]

    def norm(n):
        copies[1 + n].wait()
        step = 64
        for r in range(n * part, (n + 1) * part, step):
            v = x[r : r + step, :].astype(f32)
            shifted = v - jnp.mean(v, axis=-1, keepdims=True)
            spread = jnp.mean(shifted * shifted, axis=-1, keepdims=True)
            y = shifted * lax.rsqrt(spread + epsilon) * scale + shift
            normed[r : r + step, :] = y.astype(bf16)

    norm(0)
    copies[3].wait()
    own, left, right = slots(place, order, sections)
    targets = ((to_right, own < right), (to_left, own < left))
    copies[4].wait()

    def old_copies(n, out):
        return [
            pltpu.make_async_copy(
                held.at[i * rows : (i + 1) * rows],
                out.at[:, i * half : (i + 1) * half],
                out_sems.at[2 * n + i],
            )
            for i in range(2)
        ]

    def new_copy(n, out):
        return pltpu.make_async_copy(normed, out, out_sems.at[4 + n])

    for n, (out, fresh) in enumerate(targets):

        @pl.when(jnp.logical_not(fresh))
        def _():
            for copy in old_copies(n, out):
                copy.start()

    norm(1)
    for n, (out, fresh) in enumerate(targets):

        @pl.when(fresh)
        def _():
            new_copy(n, out).start()

    last = [pltpu.make_async_copy(normed, normed_out, out_sems.at[6])]
    last[0].start()
    copies[5].wait()
    last.append(pltpu.make_async_copy(values, values_out, out_sems.at[7]))
    last[1].start()
    for n, (out, fresh) in enumerate(targets):

        @pl.when(jnp.logical_not(fresh))
        def _():
            for copy in old_copies(n, out):
                copy.wait()

        @pl.when(fresh)
        def _():
            new_copy(n, out).wait()

    for copy in last:
        copy.wait()


def attend(queries, keys, vbuf):
    s = lax.dot_general(queries, keys, (((1,), (1,)), ((), ())), preferred_element_type=f32)
    return jnp.dot(jnp.exp2(s).astype(bf16), vbuf, preferred_element_type=f32)


def own_rows_kernel(half, weight, gains, cache, keys, key_weight, value_weight, sems):
    width = keys.shape[1]
    block = 2 * gains.shape[1]
    gain = gain_row(gains, 1)
    buffers = {2: value_weight, 1: key_weight}
    pieces = ((2, 0, block), (2, block, width), (1, 0, width))
    copies = []
    for n, (c, low, high) in enumerate(pieces):
        copy = pltpu.make_async_copy(
            weight.at[c, :, low:high], buffers[c].at[:, low:high], sems.at[n]
        )
        copy.start()
        copies.append(copy)
    for n, (c, low, high) in enumerate(pieces):
        copies[n].wait()
        for j in range(low, high, block):
            cols = slice(j, j + block)
            y = jnp.dot(half[...], buffers[c][:, cols], preferred_element_type=f32)
            y = y.astype(bf16)
            cache[c - 1, :, cols] = y
            if c == 1:
                keys[:, cols] = heads_normed(y.astype(f32), gain)


def other_rows_kernel(
    place, side, own_half, half, own_cache, own_keys, key_weight, value_weight, weight, gains,
    keep, cache, queries, keys, vbuf, query_weight, sem,
):
    load = pltpu.make_async_copy(weight.at[0], query_weight, sem)
    load.start()
    rows = half.shape[0]
    width = keys.shape[1]
    size = gains.shape[1]
    block = 2 * size
    h = side[0]
    at = pl.ds(pl.multiple_of((1 - h) * rows, rows), rows)
    own_at = pl.ds(pl.multiple_of(h * rows, rows), rows)
    mask = mask_columns((keep[pl.ds(place[0], 1), :] > 0).astype(f32), size)
    for i in range(width // size):
        vbuf[i, :, size:] = mask
    cache[:, own_at, :] = own_cache[...]
    keys[own_at, :] = own_keys[...]
    gain = gain_row(gains, 1)
    for j in range(0, width, block):
        cols = slice(j, j + block)
        y = jnp.dot(half[...], value_weight[:, cols], preferred_element_type=f32).astype(bf16)
        cache[1, at, cols] = y
        for low in range(0, block, size):
            i = (j + low) // size
            vbuf[i, at, :size] = y[:, low : low + size] * vbuf[0, at, size:]
            vbuf[i, own_at, :size] = (
                own_cache[1, :, i * size : (i + 1) * size] * vbuf[0, own_at, size:]
            )
    for j in range(0, width, block):
        cols = slice(j, j + block)
        y = jnp.dot(half[...], key_weight[:, cols], preferred_element_type=f32).astype(bf16)
        cache[0, at, cols] = y
        keys[at, cols] = heads_normed(y.astype(f32), gain)
    gain = gain_row(gains, 0) * (math.log2(math.e) * size**-0.5)
    load.wait()
    for j in range(0, width, block):
        cols = slice(j, j + block)
        for source, rows_at in ((own_half, own_at), (half, at)):
            y = jnp.dot(source[...], query_weight[:, cols], preferred_element_type=f32)
            queries[rows_at, cols] = heads_normed(y, gain)


def own_kernel(count, queries, keys, vbuf, text_in, gains, total, text, text_keys, tbuf, sem):
    load = pltpu.make_async_copy(text_in, text, sem)
    load.start()
    heads, _, wide = vbuf.shape
    size = wide // 2
    text_rows = text.shape[1]
    for i in range(heads):
        cols = slice(i * size, (i + 1) * size)
        total[:, wide * i : wide * (i + 1)] = attend(queries[:, cols], keys[:, cols], vbuf[i])
    live = lax.broadcasted_iota(jnp.int32, (text_rows, size), 0) < count[0]
    mask = live.astype(f32).astype(bf16)
    gain = gain_row(gains, 2)
    load.wait()
    for i in range(heads):
        cols = slice(i * size, (i + 1) * size)
        text_keys[:, cols] = head_normed(text[0, :, cols].astype(f32), gain)
        tbuf[i, :, :size] = text[1, :, cols] * mask
        tbuf[i, :, size:] = mask
        total[:, wide * i : wide * (i + 1)] += attend(queries[:, cols], text_keys[:, cols], tbuf[i])


def side_mask(keep, place, sections, by, size):
    wanted = place[0] + by
    there = (wanted >= 0) & (wanted < sections)
    row = keep[pl.ds(jnp.clip(wanted, 0, sections - 1), 1), :]
    return mask_columns(((row > 0) & there).astype(f32), size)


def add_side(queries, keys, vbuf, total, size):
    for i in range(queries.shape[1] // size):
        cols = slice(i * size, (i + 1) * size)
        wide = slice(2 * i * size, 2 * (i + 1) * size)
        total[:, wide] += attend(queries[:, cols], keys[:, cols], vbuf[i])


def fresh_kernel(
    sections,
    place,
    side,
    order,
    left_own,
    left_other,
    right_own,
    right_other,
    key_weight,
    value_weight,
    gains,
    queries,
    keep,
    total_in,
    total,
    keys,
    vbuf,
):
    rows = left_own.shape[0]
    _, width = queries.shape
    size = gains.shape[1]
    block = 2 * size
    h = side[0]
    own, left, right = slots(place, order, sections)
    gain = gain_row(gains, 1)
    total[...] = total_in[...]
    for mine, other, fresh, by in (
        (left_own, left_other, left < own, -1),
        (right_own, right_other, right < own, 1),
    ):

        @pl.when(fresh)
        def _():
            mask = side_mask(keep, place, sections, by, size)
            for i in range(width // size):
                vbuf[i, :, size:] = mask
            for half, at in ((mine, h), (other, 1 - h)):
                at = pl.ds(pl.multiple_of(at * rows, rows), rows)
                for j in range(0, width, block):
                    cols = slice(j, j + block)
                    y = jnp.dot(half[...], key_weight[:, cols], preferred_element_type=f32)
                    keys[at, cols] = heads_normed(y.astype(bf16).astype(f32), gain)
                for j in range(0, width, block):
                    cols = slice(j, j + block)
                    y = jnp.dot(half[...], value_weight[:, cols], preferred_element_type=f32)
                    y = y.astype(bf16)
                    for i in range(block // size):
                        vbuf[j // size + i, at, :size] = (
                            y[:, i * size : (i + 1) * size] * vbuf[0, at, size:]
                        )
            add_side(queries, keys, vbuf, total, size)


def stale_kernel(
    sections,
    place,
    side,
    order,
    left_keys,
    left_values,
    right_keys,
    right_values,
    gains,
    queries,
    keep,
    total_in,
    weight,
    sent,
    mine,
    keys,
    vbuf,
    total,
    att,
):
    rows = sent.shape[0]
    patch, width = queries.shape
    size = gains.shape[1]
    p = place[0]
    h = side[0]
    own, left, right = slots(place, order, sections)
    gain = gain_row(gains, 1)
    total[...] = total_in[...]
    for raw, values, wanted, by in (
        (left_keys, left_values, (left > own) & (p > 0), -1),
        (right_keys, right_values, (right > own) & (p < sections - 1), 1),
    ):

        @pl.when(wanted)
        def _():
            mask = side_mask(keep, place, sections, by, size)
            for r in range(patch // rows):
                keys[r * rows : (r + 1) * rows, :] = heads_normed(
                    raw[:, r * width : (r + 1) * width].astype(f32), gain
                )
            for i in range(width // size):
                cols = slice(i * size, (i + 1) * size)
                vbuf[i, :, size:] = mask
                vbuf[i, :, :size] = values[:, cols] * mask
            add_side(queries, keys, vbuf, total, size)

    for i in range(width // size):
        low = 2 * i * size
        att[:, i * size : (i + 1) * size] = (
            total[:, low : low + size] / total[:, low + size : low + 2 * size]
        ).astype(bf16)
    at = pl.ds(pl.multiple_of((1 - h) * rows, rows), rows)
    sent[...] = jnp.dot(att[at, :], weight[...], preferred_element_type=f32).astype(bf16)
    mine[...] = att[pl.ds(pl.multiple_of(h * rows, rows), rows), :]


def kept_kernel(mine, weight, kept):
    kept[...] = jnp.dot(mine[...], weight[...], preferred_element_type=f32).astype(bf16)


def swapped(array):
    return lax.ppermute(array, "head", [(0, 1), (1, 0)])


def from_behind(array, axis, by):
    count = lax.axis_size(axis)
    pairs = [(i, i + by) for i in range(count) if 0 <= i + by < count]
    return lax.ppermute(array, axis, pairs)


def on_device(
    video_tokens,
    modulation,
    project_weight,
    output_weight,
    norm_gains,
    text_cache,
    text_count,
    video_keep,
    patch_order,
    stale_cache,
):
    sections = lax.axis_size("section")
    place = lax.axis_index("section").astype(jnp.int32).reshape(1)
    side = lax.axis_index("head").astype(jnp.int32).reshape(1)
    rows, model = video_tokens.shape
    size = norm_gains.shape[1]
    width = project_weight.shape[2]
    heads = width // size
    patch = stale_cache.shape[1]
    text_rows = text_cache.shape[1]
    keep = video_keep.reshape(sections, patch)
    half_shape = jax.ShapeDtypeStruct((rows, model), bf16)
    side_shape = jax.ShapeDtypeStruct((patch, width), bf16)
    part_shape = jax.ShapeDtypeStruct((rows, width), bf16)
    total_shape = jax.ShapeDtypeStruct((patch, 2 * width), f32)
    stale_cache = in_hbm(stale_cache)

    normed, to_right, to_left, values = pl.pallas_call(
        functools.partial(first_kernel, sections),
        out_shape=(half_shape, half_shape, half_shape, side_shape),
        in_specs=[SMEM, HBM, HBM, HBM, HBM],
        out_specs=(HBM,) * 4,
        scratch_shapes=[
            pltpu.SMEM(patch_order.shape, jnp.int32),
            pltpu.VMEM((rows, model), bf16),
            pltpu.VMEM(modulation.shape, f32),
            pltpu.VMEM((patch, width), bf16),
            pltpu.VMEM((patch, width), bf16),
            pltpu.VMEM((rows, model), bf16),
            pltpu.SemaphoreType.DMA((6,)),
            pltpu.SemaphoreType.DMA((8,)),
        ],
        compiler_params=params(10),
        cost_estimate=cost(10 * rows * model, 10 * rows * model),
        name="first",
    )(place, in_hbm(patch_order), in_hbm(video_tokens), in_hbm(modulation), stale_cache)

    left_own = from_behind(to_right, "section", 1)
    right_own = from_behind(to_left, "section", -1)
    left_values = from_behind(values, "section", 1)
    right_values = from_behind(values, "section", -1)
    other = swapped(normed)

    weight_shape = jax.ShapeDtypeStruct((model, width), bf16)
    project_weight = in_hbm(project_weight)
    own_cache, own_keys, key_weight, value_weight = pl.pallas_call(
        own_rows_kernel,
        out_shape=(
            jax.ShapeDtypeStruct((2, rows, width), bf16),
            part_shape,
            weight_shape,
            weight_shape,
        ),
        in_specs=[VMEM, HBM, VMEM],
        out_specs=(VMEM,) * 4,
        scratch_shapes=[pltpu.SemaphoreType.DMA((3,))],
        compiler_params=params(10),
        cost_estimate=cost(4 * rows * model * width, 4 * rows * width),
        name="own_rows",
    )(normed, project_weight, norm_gains)

    fresh_cache, queries, keys, vbuf = pl.pallas_call(
        other_rows_kernel,
        out_shape=(
            jax.ShapeDtypeStruct((2, patch, width), bf16),
            side_shape,
            side_shape,
            jax.ShapeDtypeStruct((heads, patch, 2 * size), bf16),
        ),
        in_specs=[SMEM, SMEM] + [VMEM] * 6 + [HBM, VMEM, VMEM],
        out_specs=(VMEM,) * 4,
        scratch_shapes=[pltpu.VMEM((model, width), bf16), pltpu.SemaphoreType.DMA],
        compiler_params=params(16),
        cost_estimate=cost(8 * rows * model * width, 4 * rows * width),
        name="other_rows",
    )(
        place,
        side,
        normed,
        other,
        own_cache,
        own_keys,
        key_weight,
        value_weight,
        project_weight,
        norm_gains,
        keep,
    )

    left_own, right_own, queries = lax.optimization_barrier((left_own, right_own, queries))
    left_other = swapped(left_own)
    right_other = swapped(right_own)

    total = pl.pallas_call(
        own_kernel,
        out_shape=total_shape,
        in_specs=[SMEM, VMEM, VMEM, VMEM, HBM, VMEM],
        out_specs=VMEM,
        scratch_shapes=[
            pltpu.VMEM((2, text_rows, width), bf16),
            pltpu.VMEM((text_rows, width), bf16),
            pltpu.VMEM((heads, text_rows, 2 * size), bf16),
            pltpu.SemaphoreType.DMA,
        ],
        compiler_params=params(12),
        cost_estimate=cost(6 * patch * (patch + text_rows) * width, 6 * patch * width),
        name="own",
    )(text_count, queries, keys, vbuf, in_hbm(text_cache), norm_gains)

    total = pl.pallas_call(
        functools.partial(fresh_kernel, sections),
        out_shape=total_shape,
        in_specs=[SMEM] * 3 + [VMEM] * 10,
        out_specs=VMEM,
        scratch_shapes=[
            pltpu.VMEM((patch, width), bf16),
            pltpu.VMEM((heads, patch, 2 * size), bf16),
        ],
        input_output_aliases={12: 0},
        compiler_params=params(24),
        cost_estimate=cost(4 * patch * model * width, 6 * patch * width),
        name="fresh",
    )(
        place,
        side,
        patch_order,
        left_own,
        left_other,
        right_own,
        right_other,
        key_weight,
        value_weight,
        norm_gains,
        queries,
        keep,
        total,
    )

    sent, mine = pl.pallas_call(
        functools.partial(stale_kernel, sections),
        out_shape=(half_shape, part_shape),
        in_specs=[SMEM] * 3 + [VMEM] * 9,
        out_specs=(VMEM, VMEM),
        scratch_shapes=[
            pltpu.VMEM((patch, width), bf16),
            pltpu.VMEM((heads, patch, 2 * size), bf16),
            pltpu.VMEM((patch, 2 * width), f32),
            pltpu.VMEM((patch, width), bf16),
        ],
        compiler_params=params(24),
        cost_estimate=cost(2 * patch * width * model, 6 * patch * width),
        name="stale",
    )(
        place,
        side,
        patch_order,
        left_own,
        left_values,
        right_own,
        right_values,
        norm_gains,
        queries,
        keep,
        total,
        output_weight,
    )
    received = swapped(sent)
    kept = pl.pallas_call(
        kept_kernel,
        out_shape=half_shape,
        in_specs=[VMEM, VMEM],
        out_specs=VMEM,
        compiler_params=params(8),
        cost_estimate=cost(2 * rows * width * model, 4 * rows * model),
        name="kept",
    )(mine, output_weight)
    mixed = kept.astype(f32) + received.astype(f32)
    updated = (video_tokens.astype(f32) + modulation[2] * mixed).astype(bf16)
    return (updated, fresh_cache)


def solution(mesh):
    placed = (
        P(("groups", "section", "head"), None),
        P("groups", None),
        P(None, None, "head"),
        P("head", None),
        P(),
        P(None, "groups", "head"),
        P("groups"),
        P("groups"),
        P("groups"),
        P(None, ("groups", "section"), "head"),
    )

    return jax.shard_map(
        on_device,
        mesh=mesh,
        in_specs=placed,
        out_specs=(P(("groups", "section", "head"), None), P(None, ("groups", "section"), "head")),
        check_vma=False,
    )
```

```python
import functools
import math

import jax
import jax.numpy as jnp
from jax import lax
from jax.experimental import pallas as pl
from jax.experimental.pallas import tpu as pltpu
from jax.sharding import PartitionSpec as P


epsilon = 1e-06
f32 = jnp.float32
bf16 = jnp.bfloat16
MIB = 1024 * 1024

VMEM = pl.BlockSpec(memory_space=pltpu.VMEM)
SMEM = pl.BlockSpec(memory_space=pltpu.SMEM)
HBM = pl.BlockSpec(memory_space=pltpu.HBM)


def params(mib):
    return pltpu.CompilerParams(vmem_limit_bytes=mib * MIB)


def in_hbm(array):
    return pltpu.with_memory_space_constraint(array, pltpu.HBM)


def cost(flops, nbytes):
    return pl.CostEstimate(flops=flops, bytes_accessed=nbytes, transcendentals=0)


def partners(place, sections):
    p = place[0]
    by = 2 * lax.rem(p, 2) - 1
    return tuple(jnp.clip(q, 0, sections - 1) for q in (p + by, p - by))


def gain_row(gains, which):
    return gains[which : which + 1, :]


def head_normed(part, gain):
    spread = jnp.mean(part * part, axis=-1, keepdims=True)
    return (part * lax.rsqrt(spread + epsilon) * gain).astype(bf16)


def heads_normed(part, gain):
    size = gain.shape[-1]
    pieces = [
        head_normed(part[:, i : i + size], gain) for i in range(0, part.shape[-1], size)
    ]
    return jnp.concatenate(pieces, axis=-1)


def mask_columns(row, lanes):
    return jnp.broadcast_to(row, (lanes, row.shape[1])).T.astype(bf16)


def first_kernel(
    sections, place, order_in, x_in, mod_in, stale, normed_out, to_odd, to_even, values_out,
    order, x, mod, held, values, normed, sems, out_sems,
):
    rows, width = x.shape
    part = rows // 2
    half = width // 2
    loads = [(mod_in, mod)] + [(x_in.at[r : r + part], x.at[r : r + part]) for r in (0, part)]
    loads += [(order_in, order), (stale.at[0], held), (stale.at[1], values)]
    copies = [
        pltpu.make_async_copy(source, target, sems.at[i])
        for i, (source, target) in enumerate(loads)
    ]
    for copy in copies:
        copy.start()
    copies[0].wait()
    scale = 1.0 + mod[1:2, :]
    shift = mod[0:1, :]

    def norm(n):
        copies[1 + n].wait()
        step = 64
        for r in range(n * part, (n + 1) * part, step):
            v = x[r : r + step, :].astype(f32)
            shifted = v - jnp.mean(v, axis=-1, keepdims=True)
            spread = jnp.mean(shifted * shifted, axis=-1, keepdims=True)
            y = shifted * lax.rsqrt(spread + epsilon) * scale + shift
            normed[r : r + step, :] = y.astype(bf16)

    norm(0)
    copies[3].wait()
    own = order[place[0]]
    targets = tuple(
        (out, own < order[q]) for out, q in zip((to_odd, to_even), partners(place, sections))
    )
    copies[4].wait()

    def old_copies(n, out):
        return [
            pltpu.make_async_copy(
                held.at[i * rows : (i + 1) * rows],
                out.at[:, i * half : (i + 1) * half],
                out_sems.at[2 * n + i],
            )
            for i in range(2)
        ]

    def new_copy(n, out):
        return pltpu.make_async_copy(normed, out, out_sems.at[4 + n])

    for n, (out, fresh) in enumerate(targets):

        @pl.when(jnp.logical_not(fresh))
        def _():
            for copy in old_copies(n, out):
                copy.start()

    norm(1)
    for n, (out, fresh) in enumerate(targets):

        @pl.when(fresh)
        def _():
            new_copy(n, out).start()

    last = [pltpu.make_async_copy(normed, normed_out, out_sems.at[6])]
    last[0].start()
    copies[5].wait()
    last.append(pltpu.make_async_copy(values, values_out, out_sems.at[7]))
    last[1].start()
    for n, (out, fresh) in enumerate(targets):

        @pl.when(jnp.logical_not(fresh))
        def _():
            for copy in old_copies(n, out):
                copy.wait()

        @pl.when(fresh)
        def _():
            new_copy(n, out).wait()

    for copy in last:
        copy.wait()


def attend(queries, keys, vbuf):
    s = lax.dot_general(queries, keys, (((1,), (1,)), ((), ())), preferred_element_type=f32)
    return jnp.dot(jnp.exp2(s).astype(bf16), vbuf, preferred_element_type=f32)


def own_rows_kernel(half, weight, gains, cache, keys, key_weight, value_weight, sems):
    width = keys.shape[1]
    block = 2 * gains.shape[1]
    gain = gain_row(gains, 1)
    buffers = {2: value_weight, 1: key_weight}
    pieces = ((2, 0, block), (2, block, width), (1, 0, width))
    copies = []
    for n, (c, low, high) in enumerate(pieces):
        copy = pltpu.make_async_copy(
            weight.at[c, :, low:high], buffers[c].at[:, low:high], sems.at[n]
        )
        copy.start()
        copies.append(copy)
    for n, (c, low, high) in enumerate(pieces):
        copies[n].wait()
        for j in range(low, high, block):
            cols = slice(j, j + block)
            y = jnp.dot(half[...], buffers[c][:, cols], preferred_element_type=f32)
            y = y.astype(bf16)
            cache[c - 1, :, cols] = y
            if c == 1:
                keys[:, cols] = heads_normed(y.astype(f32), gain)


def other_rows_kernel(
    place, side, own_half, half_in, own_cache, own_keys, key_weight, value_weight, weight, gains,
    keep, cache, queries, keys, vbuf, half, raw, query_weight, sems,
):
    load_half = pltpu.make_async_copy(half_in, half, sems.at[0])
    load_half.start()
    load_weight = pltpu.make_async_copy(weight.at[0], query_weight, sems.at[1])
    load_weight.start()
    rows = half.shape[0]
    width = keys.shape[1]
    size = gains.shape[1]
    block = 2 * size
    h = side[0]
    at = pl.ds(pl.multiple_of((1 - h) * rows, rows), rows)
    own_at = pl.ds(pl.multiple_of(h * rows, rows), rows)
    stores = [
        pltpu.make_async_copy(own_cache, cache.at[:, own_at, :], sems.at[2]),
        pltpu.make_async_copy(raw.at[1], cache.at[1, at, :], sems.at[3]),
        pltpu.make_async_copy(raw.at[0], cache.at[0, at, :], sems.at[4]),
    ]
    stores[0].start()
    mask = mask_columns((keep[pl.ds(place[0], 1), :] > 0).astype(f32), size)
    for i in range(width // size):
        vbuf[i, :, size:] = mask
    keys[own_at, :] = own_keys[...]
    for i in range(width // size):
        vbuf[i, own_at, :size] = (
            own_cache[1, :, i * size : (i + 1) * size] * vbuf[0, own_at, size:]
        )
    gain = gain_row(gains, 1)
    load_half.wait()
    for j in range(0, width, block):
        cols = slice(j, j + block)
        y = jnp.dot(half[...], value_weight[:, cols], preferred_element_type=f32).astype(bf16)
        raw[1, :, cols] = y
        for low in range(0, block, size):
            vbuf[(j + low) // size, at, :size] = y[:, low : low + size] * vbuf[0, at, size:]
    for j in range(0, width, block):
        cols = slice(j, j + block)
        y = jnp.dot(half[...], key_weight[:, cols], preferred_element_type=f32).astype(bf16)
        raw[0, :, cols] = y
        keys[at, cols] = heads_normed(y.astype(f32), gain)
    gain = gain_row(gains, 0) * (math.log2(math.e) * size**-0.5)
    load_weight.wait()
    stores[1].start()
    stores[2].start()
    for j in range(0, width, block):
        cols = slice(j, j + block)
        for source, rows_at in ((own_half, own_at), (half, at)):
            y = jnp.dot(source[...], query_weight[:, cols], preferred_element_type=f32)
            queries[rows_at, cols] = heads_normed(y, gain)
    for store in stores:
        store.wait()


def own_kernel(count, queries, keys, vbuf, text_in, gains, total, text, text_keys, tbuf, sem):
    load = pltpu.make_async_copy(text_in, text, sem)
    load.start()
    heads, _, wide = vbuf.shape
    size = wide // 2
    text_rows = text.shape[1]
    for i in range(heads):
        cols = slice(i * size, (i + 1) * size)
        total[:, wide * i : wide * (i + 1)] = attend(queries[:, cols], keys[:, cols], vbuf[i])
    live = lax.broadcasted_iota(jnp.int32, (text_rows, size), 0) < count[0]
    mask = live.astype(f32).astype(bf16)
    gain = gain_row(gains, 2)
    load.wait()
    for i in range(heads):
        cols = slice(i * size, (i + 1) * size)
        text_keys[:, cols] = head_normed(text[0, :, cols].astype(f32), gain)
        tbuf[i, :, :size] = text[1, :, cols] * mask
        tbuf[i, :, size:] = mask
        total[:, wide * i : wide * (i + 1)] += attend(queries[:, cols], text_keys[:, cols], tbuf[i])


def side_mask(keep, wanted, size):
    return mask_columns((keep[pl.ds(wanted, 1), :] > 0).astype(f32), size)


def near_kernel(
    sections,
    place,
    side,
    order,
    odd_own,
    odd_other,
    even_own,
    even_other,
    key_weight,
    value_weight,
    gains,
    queries,
    keep,
    total_in,
    total,
    weights,
    keys,
    vbuf,
):
    rows = odd_own.shape[0]
    patch, width = queries.shape
    size = gains.shape[1]
    block = 2 * size
    heads = width // size
    h = side[0]
    own = order[place[0]]
    gain = gain_row(gains, 1)
    total[...] = total_in[...]
    sources = ((odd_own, odd_other), (even_own, even_other))
    for n, ((mine, other), q) in enumerate(zip(sources, partners(place, sections))):

        @pl.when(order[q] < own)
        def _():
            mask = side_mask(keep, q, size)
            for i in range(heads):
                vbuf[i, :, size:] = mask
            for half, at in ((mine, h), (other, 1 - h)):
                at = pl.ds(pl.multiple_of(at * rows, rows), rows)
                for j in range(0, width, block):
                    cols = slice(j, j + block)
                    y = jnp.dot(half[...], key_weight[:, cols], preferred_element_type=f32)
                    keys[at, cols] = heads_normed(y.astype(bf16).astype(f32), gain)
                for j in range(0, width, block):
                    cols = slice(j, j + block)
                    y = jnp.dot(half[...], value_weight[:, cols], preferred_element_type=f32)
                    y = y.astype(bf16)
                    for low in range(0, block, size):
                        vbuf[(j + low) // size, at, :size] = (
                            y[:, low : low + size] * vbuf[0, at, size:]
                        )
            for i in range(heads):
                cols = slice(i * size, (i + 1) * size)
                wide = slice(2 * i * size, 2 * (i + 1) * size)
                total[:, wide] += attend(queries[:, cols], keys[:, cols], vbuf[i])

        @pl.when(order[q] > own)
        def _():
            for r in range(patch // rows):
                keys[r * rows : (r + 1) * rows, :] = heads_normed(
                    mine[:, r * width : (r + 1) * width].astype(f32), gain
                )
            for i in range(heads):
                cols = slice(i * size, (i + 1) * size)
                s = lax.dot_general(
                    queries[:, cols],
                    keys[:, cols],
                    (((1,), (1,)), ((), ())),
                    preferred_element_type=f32,
                )
                weights[n, i] = jnp.exp2(s).astype(bf16)


def finish_kernel(
    sections,
    flip,
    place,
    side,
    order,
    weights,
    odd_values,
    even_values,
    keep,
    total,
    weight,
    out,
    vbuf,
    sums,
    att,
):
    rows = out.shape[0]
    heads = vbuf.shape[0]
    size = vbuf.shape[2] // 2
    h = side[0]
    at = pl.ds(pl.multiple_of((1 - h if flip else h) * rows, rows), rows)
    own = order[place[0]]
    sums[...] = total[at, :]
    for n, (values, q) in enumerate(zip((odd_values, even_values), partners(place, sections))):

        @pl.when(order[q] > own)
        def _():
            mask = side_mask(keep, q, size)
            for i in range(heads):
                vbuf[i, :, size:] = mask
                vbuf[i, :, :size] = values[:, i * size : (i + 1) * size] * mask
                sums[:, 2 * i * size : 2 * (i + 1) * size] += jnp.dot(
                    weights[n, i, at, :], vbuf[i], preferred_element_type=f32
                )

    for i in range(heads):
        low = 2 * i * size
        att[:, i * size : (i + 1) * size] = (
            sums[:, low : low + size] / sums[:, low + size : low + 2 * size]
        ).astype(bf16)
    out[...] = jnp.dot(att[...], weight[...], preferred_element_type=f32).astype(bf16)


def swapped(array):
    return lax.ppermute(array, "head", [(0, 1), (1, 0)])


def across(array, first):
    count = lax.axis_size("section")
    edges = [(i, i + 1) for i in range(first, count - 1, 2)]
    return lax.ppermute(array, "section", edges + [(j, i) for i, j in edges])


def on_device(
    video_tokens,
    modulation,
    project_weight,
    output_weight,
    norm_gains,
    text_cache,
    text_count,
    video_keep,
    patch_order,
    stale_cache,
):
    sections = lax.axis_size("section")
    place = lax.axis_index("section").astype(jnp.int32).reshape(1)
    side = lax.axis_index("head").astype(jnp.int32).reshape(1)
    rows, model = video_tokens.shape
    size = norm_gains.shape[1]
    width = project_weight.shape[2]
    heads = width // size
    patch = stale_cache.shape[1]
    text_rows = text_cache.shape[1]
    keep = video_keep.reshape(sections, patch)
    half_shape = jax.ShapeDtypeStruct((rows, model), bf16)
    side_shape = jax.ShapeDtypeStruct((patch, width), bf16)
    part_shape = jax.ShapeDtypeStruct((rows, width), bf16)
    total_shape = jax.ShapeDtypeStruct((patch, 2 * width), f32)
    stale_cache = in_hbm(stale_cache)

    normed, to_odd, to_even, values = pl.pallas_call(
        functools.partial(first_kernel, sections),
        out_shape=(half_shape, half_shape, half_shape, side_shape),
        in_specs=[SMEM, HBM, HBM, HBM, HBM],
        out_specs=(HBM,) * 4,
        scratch_shapes=[
            pltpu.SMEM(patch_order.shape, jnp.int32),
            pltpu.VMEM((rows, model), bf16),
            pltpu.VMEM(modulation.shape, f32),
            pltpu.VMEM((patch, width), bf16),
            pltpu.VMEM((patch, width), bf16),
            pltpu.VMEM((rows, model), bf16),
            pltpu.SemaphoreType.DMA((6,)),
            pltpu.SemaphoreType.DMA((8,)),
        ],
        compiler_params=params(10),
        cost_estimate=cost(10 * rows * model, 10 * rows * model),
        name="first",
    )(place, in_hbm(patch_order), in_hbm(video_tokens), in_hbm(modulation), stale_cache)

    odd_own = across(to_odd, 1)
    odd_values = across(values, 1)
    even_own = across(to_even, 0)
    even_values = across(values, 0)
    other = swapped(normed)

    weight_shape = jax.ShapeDtypeStruct((model, width), bf16)
    project_weight = in_hbm(project_weight)
    own_cache, own_keys, key_weight, value_weight = pl.pallas_call(
        own_rows_kernel,
        out_shape=(
            jax.ShapeDtypeStruct((2, rows, width), bf16),
            part_shape,
            weight_shape,
            weight_shape,
        ),
        in_specs=[VMEM, HBM, VMEM],
        out_specs=(VMEM,) * 4,
        scratch_shapes=[pltpu.SemaphoreType.DMA((3,))],
        compiler_params=params(10),
        cost_estimate=cost(4 * rows * model * width, 4 * rows * width),
        name="own_rows",
    )(normed, project_weight, norm_gains)

    fresh_cache, queries, keys, vbuf = pl.pallas_call(
        other_rows_kernel,
        out_shape=(
            jax.ShapeDtypeStruct((2, patch, width), bf16),
            side_shape,
            side_shape,
            jax.ShapeDtypeStruct((heads, patch, 2 * size), bf16),
        ),
        in_specs=[SMEM, SMEM, VMEM, HBM] + [VMEM] * 4 + [HBM, VMEM, VMEM],
        out_specs=(HBM,) + (VMEM,) * 3,
        scratch_shapes=[
            pltpu.VMEM((rows, model), bf16),
            pltpu.VMEM((2, rows, width), bf16),
            pltpu.VMEM((model, width), bf16),
            pltpu.SemaphoreType.DMA((5,)),
        ],
        compiler_params=params(16),
        cost_estimate=cost(8 * rows * model * width, 4 * rows * width),
        name="other_rows",
    )(
        place,
        side,
        normed,
        in_hbm(other),
        own_cache,
        own_keys,
        key_weight,
        value_weight,
        project_weight,
        norm_gains,
        keep,
    )

    odd_own, even_own, queries = lax.optimization_barrier((odd_own, even_own, queries))
    odd_other = swapped(odd_own)
    even_other = swapped(even_own)

    total = pl.pallas_call(
        own_kernel,
        out_shape=total_shape,
        in_specs=[SMEM, VMEM, VMEM, VMEM, HBM, VMEM],
        out_specs=VMEM,
        scratch_shapes=[
            pltpu.VMEM((2, text_rows, width), bf16),
            pltpu.VMEM((text_rows, width), bf16),
            pltpu.VMEM((heads, text_rows, 2 * size), bf16),
            pltpu.SemaphoreType.DMA,
        ],
        compiler_params=params(12),
        cost_estimate=cost(6 * patch * (patch + text_rows) * width, 6 * patch * width),
        name="own",
    )(text_count, queries, keys, vbuf, in_hbm(text_cache), norm_gains)

    total, weights = pl.pallas_call(
        functools.partial(near_kernel, sections),
        out_shape=(total_shape, jax.ShapeDtypeStruct((2, heads, patch, patch), bf16)),
        in_specs=[SMEM] * 3 + [VMEM] * 10,
        out_specs=(VMEM, VMEM),
        scratch_shapes=[
            pltpu.VMEM((patch, width), bf16),
            pltpu.VMEM((heads, patch, 2 * size), bf16),
        ],
        input_output_aliases={12: 0},
        compiler_params=params(24),
        cost_estimate=cost(4 * patch * model * width, 6 * patch * width),
        name="near",
    )(
        place,
        side,
        patch_order,
        odd_own,
        odd_other,
        even_own,
        even_other,
        key_weight,
        value_weight,
        norm_gains,
        queries,
        keep,
        total,
    )

    def finish(flip):
        return pl.pallas_call(
            functools.partial(finish_kernel, sections, flip),
            out_shape=half_shape,
            in_specs=[SMEM] * 3 + [VMEM] * 6,
            out_specs=VMEM,
            scratch_shapes=[
                pltpu.VMEM((heads, patch, 2 * size), bf16),
                pltpu.VMEM((rows, 2 * width), f32),
                pltpu.VMEM((rows, width), bf16),
            ],
            compiler_params=params(20),
            cost_estimate=cost(2 * rows * width * model, 4 * rows * model),
            name="finish_sent" if flip else "finish_kept",
        )(place, side, patch_order, weights, odd_values, even_values, keep, total, output_weight)

    sent = finish(True)
    received = swapped(sent)
    kept = finish(False)
    mixed = kept.astype(f32) + received.astype(f32)
    updated = (video_tokens.astype(f32) + modulation[2] * mixed).astype(bf16)
    return (updated, fresh_cache)


def solution(mesh):
    placed = (
        P(("groups", "section", "head"), None),
        P("groups", None),
        P(None, None, "head"),
        P("head", None),
        P(),
        P(None, "groups", "head"),
        P("groups"),
        P("groups"),
        P("groups"),
        P(None, ("groups", "section"), "head"),
    )

    return jax.shard_map(
        on_device,
        mesh=mesh,
        in_specs=placed,
        out_specs=(P(("groups", "section", "head"), None), P(None, ("groups", "section"), "head")),
        check_vma=False,
    )
```

```python
import functools
import math

import jax
import jax.numpy as jnp
from jax import lax
from jax.experimental import pallas as pl
from jax.experimental.pallas import tpu as pltpu
from jax.sharding import PartitionSpec as P


epsilon = 1e-06
f32 = jnp.float32
bf16 = jnp.bfloat16
MIB = 1024 * 1024

VMEM = pl.BlockSpec(memory_space=pltpu.VMEM)
SMEM = pl.BlockSpec(memory_space=pltpu.SMEM)
HBM = pl.BlockSpec(memory_space=pltpu.HBM)


def params(mib):
    return pltpu.CompilerParams(vmem_limit_bytes=mib * MIB)


def in_hbm(array):
    return pltpu.with_memory_space_constraint(array, pltpu.HBM)


def cost(flops, nbytes):
    return pl.CostEstimate(flops=flops, bytes_accessed=nbytes, transcendentals=0)


def partners(place, sections):
    p = place[0]
    by = 2 * lax.rem(p, 2) - 1
    return tuple(jnp.clip(q, 0, sections - 1) for q in (p + by, p - by))


def gain_row(gains, which):
    return gains[which : which + 1, :]


def head_normed(part, gain):
    spread = jnp.mean(part * part, axis=-1, keepdims=True)
    return (part * lax.rsqrt(spread + epsilon) * gain).astype(bf16)


def heads_normed(part, gain):
    size = gain.shape[-1]
    pieces = [
        head_normed(part[:, i : i + size], gain) for i in range(0, part.shape[-1], size)
    ]
    return jnp.concatenate(pieces, axis=-1)


def mask_columns(row, lanes):
    return jnp.broadcast_to(row, (lanes, row.shape[1])).T.astype(bf16)


def first_kernel(
    sections, place, order_in, x_in, mod_in, stale, normed_out, to_odd, to_even, values_out,
    order, x, mod, held, values, normed, sems, out_sems,
):
    rows, width = x.shape
    part = rows // 2
    half = width // 2
    loads = [(mod_in, mod)] + [(x_in.at[r : r + part], x.at[r : r + part]) for r in (0, part)]
    loads += [(order_in, order), (stale.at[0], held), (stale.at[1], values)]
    copies = [
        pltpu.make_async_copy(source, target, sems.at[i])
        for i, (source, target) in enumerate(loads)
    ]
    for copy in copies:
        copy.start()
    copies[0].wait()
    scale = 1.0 + mod[1:2, :]
    shift = mod[0:1, :]

    def norm(n):
        copies[1 + n].wait()
        step = 64
        for r in range(n * part, (n + 1) * part, step):
            v = x[r : r + step, :].astype(f32)
            shifted = v - jnp.mean(v, axis=-1, keepdims=True)
            spread = jnp.mean(shifted * shifted, axis=-1, keepdims=True)
            y = shifted * lax.rsqrt(spread + epsilon) * scale + shift
            normed[r : r + step, :] = y.astype(bf16)

    norm(0)
    copies[3].wait()
    own = order[place[0]]
    targets = tuple(
        (out, own < order[q]) for out, q in zip((to_odd, to_even), partners(place, sections))
    )
    copies[4].wait()

    def old_copies(n, out):
        return [
            pltpu.make_async_copy(
                held.at[i * rows : (i + 1) * rows],
                out.at[:, i * half : (i + 1) * half],
                out_sems.at[2 * n + i],
            )
            for i in range(2)
        ]

    def new_copy(n, out):
        return pltpu.make_async_copy(normed, out, out_sems.at[4 + n])

    for n, (out, fresh) in enumerate(targets):

        @pl.when(jnp.logical_not(fresh))
        def _():
            for copy in old_copies(n, out):
                copy.start()

    norm(1)
    for n, (out, fresh) in enumerate(targets):

        @pl.when(fresh)
        def _():
            new_copy(n, out).start()

    last = [pltpu.make_async_copy(normed, normed_out, out_sems.at[6])]
    last[0].start()
    copies[5].wait()
    last.append(pltpu.make_async_copy(values, values_out, out_sems.at[7]))
    last[1].start()
    for n, (out, fresh) in enumerate(targets):

        @pl.when(jnp.logical_not(fresh))
        def _():
            for copy in old_copies(n, out):
                copy.wait()

        @pl.when(fresh)
        def _():
            new_copy(n, out).wait()

    for copy in last:
        copy.wait()


def attend(queries, keys, vbuf):
    s = lax.dot_general(queries, keys, (((1,), (1,)), ((), ())), preferred_element_type=f32)
    return jnp.dot(jnp.exp2(s).astype(bf16), vbuf, preferred_element_type=f32)


def own_rows_kernel(
    half, weight, gains_in, cache, keys, key_weight, value_weight, gains, sems, gains_sem
):
    load_gains = pltpu.make_async_copy(gains_in, gains, gains_sem)
    load_gains.start()
    width = keys.shape[1]
    block = 2 * gains.shape[1]
    buffers = {2: value_weight, 1: key_weight}
    pieces = ((2, 0, block), (2, block, width), (1, 0, width))
    copies = []
    for n, (c, low, high) in enumerate(pieces):
        copy = pltpu.make_async_copy(
            weight.at[c, :, low:high], buffers[c].at[:, low:high], sems.at[n]
        )
        copy.start()
        copies.append(copy)
    load_gains.wait()
    gain = gain_row(gains, 1)
    for n, (c, low, high) in enumerate(pieces):
        copies[n].wait()
        for j in range(low, high, block):
            cols = slice(j, j + block)
            y = jnp.dot(half[...], buffers[c][:, cols], preferred_element_type=f32)
            y = y.astype(bf16)
            cache[c - 1, :, cols] = y
            if c == 1:
                keys[:, cols] = heads_normed(y.astype(f32), gain)


def other_rows_kernel(
    place, side, own_half, half_in, own_cache, own_keys, key_weight, value_weight, weight, gains,
    keep, cache, queries, keys, vbuf, half, raw, query_weight, sems,
):
    load_half = pltpu.make_async_copy(half_in, half, sems.at[0])
    load_half.start()
    load_weight = pltpu.make_async_copy(weight.at[0], query_weight, sems.at[1])
    load_weight.start()
    rows = half.shape[0]
    width = keys.shape[1]
    size = gains.shape[1]
    block = 2 * size
    h = side[0]
    at = pl.ds(pl.multiple_of((1 - h) * rows, rows), rows)
    own_at = pl.ds(pl.multiple_of(h * rows, rows), rows)
    stores = [
        pltpu.make_async_copy(own_cache, cache.at[:, own_at, :], sems.at[2]),
        pltpu.make_async_copy(raw.at[1], cache.at[1, at, :], sems.at[3]),
        pltpu.make_async_copy(raw.at[0], cache.at[0, at, :], sems.at[4]),
    ]
    stores[0].start()
    mask = mask_columns((keep[pl.ds(place[0], 1), :] > 0).astype(f32), size)
    for i in range(width // size):
        vbuf[i, :, size:] = mask
    keys[own_at, :] = own_keys[...]
    for i in range(width // size):
        vbuf[i, own_at, :size] = (
            own_cache[1, :, i * size : (i + 1) * size] * vbuf[0, own_at, size:]
        )
    gain = gain_row(gains, 1)
    load_half.wait()
    for j in range(0, width, block):
        cols = slice(j, j + block)
        y = jnp.dot(half[...], value_weight[:, cols], preferred_element_type=f32).astype(bf16)
        raw[1, :, cols] = y
        for low in range(0, block, size):
            vbuf[(j + low) // size, at, :size] = y[:, low : low + size] * vbuf[0, at, size:]
    for j in range(0, width, block):
        cols = slice(j, j + block)
        y = jnp.dot(half[...], key_weight[:, cols], preferred_element_type=f32).astype(bf16)
        raw[0, :, cols] = y
        keys[at, cols] = heads_normed(y.astype(f32), gain)
    gain = gain_row(gains, 0) * (math.log2(math.e) * size**-0.5)
    load_weight.wait()
    stores[1].start()
    stores[2].start()
    for j in range(0, width, block):
        cols = slice(j, j + block)
        for source, rows_at in ((own_half, own_at), (half, at)):
            y = jnp.dot(source[...], query_weight[:, cols], preferred_element_type=f32)
            queries[rows_at, cols] = heads_normed(y, gain)
    for store in stores:
        store.wait()


def own_kernel(count, queries, keys, vbuf, text_in, gains, total, text, text_keys, tbuf, sem):
    load = pltpu.make_async_copy(text_in, text, sem)
    load.start()
    heads, _, wide = vbuf.shape
    size = wide // 2
    text_rows = text.shape[1]
    for i in range(heads):
        cols = slice(i * size, (i + 1) * size)
        total[:, wide * i : wide * (i + 1)] = attend(queries[:, cols], keys[:, cols], vbuf[i])
    live = lax.broadcasted_iota(jnp.int32, (text_rows, size), 0) < count[0]
    mask = live.astype(f32).astype(bf16)
    gain = gain_row(gains, 2)
    load.wait()
    for i in range(heads):
        cols = slice(i * size, (i + 1) * size)
        text_keys[:, cols] = head_normed(text[0, :, cols].astype(f32), gain)
        tbuf[i, :, :size] = text[1, :, cols] * mask
        tbuf[i, :, size:] = mask
        total[:, wide * i : wide * (i + 1)] += attend(queries[:, cols], text_keys[:, cols], tbuf[i])


def side_mask(keep, wanted, size):
    return mask_columns((keep[pl.ds(wanted, 1), :] > 0).astype(f32), size)


def near_kernel(
    sections,
    edge,
    place,
    side,
    order,
    mine,
    other,
    key_weight,
    value_weight,
    gains,
    queries,
    keep,
    total_in,
    total,
    weights,
    keys,
    vbuf,
):
    rows = mine.shape[0]
    patch, width = queries.shape
    size = gains.shape[1]
    block = 2 * size
    heads = width // size
    h = side[0]
    own = order[place[0]]
    q = partners(place, sections)[edge]
    gain = gain_row(gains, 1)
    total[...] = total_in[...]

    @pl.when(order[q] < own)
    def _():
        mask = side_mask(keep, q, size)
        for i in range(heads):
            vbuf[i, :, size:] = mask
        for half, at in ((mine, h), (other, 1 - h)):
            at = pl.ds(pl.multiple_of(at * rows, rows), rows)
            for j in range(0, width, block):
                cols = slice(j, j + block)
                y = jnp.dot(half[...], key_weight[:, cols], preferred_element_type=f32)
                keys[at, cols] = heads_normed(y.astype(bf16).astype(f32), gain)
            for j in range(0, width, block):
                cols = slice(j, j + block)
                y = jnp.dot(half[...], value_weight[:, cols], preferred_element_type=f32)
                y = y.astype(bf16)
                for low in range(0, block, size):
                    vbuf[(j + low) // size, at, :size] = (
                        y[:, low : low + size] * vbuf[0, at, size:]
                    )
        for i in range(heads):
            cols = slice(i * size, (i + 1) * size)
            wide = slice(2 * i * size, 2 * (i + 1) * size)
            total[:, wide] += attend(queries[:, cols], keys[:, cols], vbuf[i])

    @pl.when(order[q] > own)
    def _():
        for r in range(patch // rows):
            keys[r * rows : (r + 1) * rows, :] = heads_normed(
                mine[:, r * width : (r + 1) * width].astype(f32), gain
            )
        for i in range(heads):
            cols = slice(i * size, (i + 1) * size)
            s = lax.dot_general(
                queries[:, cols],
                keys[:, cols],
                (((1,), (1,)), ((), ())),
                preferred_element_type=f32,
            )
            weights[i] = jnp.exp2(s).astype(bf16)


def finish_kernel(
    sections,
    flip,
    place,
    side,
    order,
    odd_weights,
    even_weights,
    odd_values,
    even_values,
    keep,
    total,
    weight,
    out,
    vbuf,
    sums,
    att,
):
    rows = out.shape[0]
    heads = vbuf.shape[0]
    size = vbuf.shape[2] // 2
    h = side[0]
    at = pl.ds(pl.multiple_of((1 - h if flip else h) * rows, rows), rows)
    own = order[place[0]]
    sums[...] = total[at, :]
    odd, even = partners(place, sections)
    for weights, values, q in ((odd_weights, odd_values, odd), (even_weights, even_values, even)):

        @pl.when(order[q] > own)
        def _():
            mask = side_mask(keep, q, size)
            for i in range(heads):
                vbuf[i, :, size:] = mask
                vbuf[i, :, :size] = values[:, i * size : (i + 1) * size] * mask
                sums[:, 2 * i * size : 2 * (i + 1) * size] += jnp.dot(
                    weights[i, at, :], vbuf[i], preferred_element_type=f32
                )

    for i in range(heads):
        low = 2 * i * size
        att[:, i * size : (i + 1) * size] = (
            sums[:, low : low + size] / sums[:, low + size : low + 2 * size]
        ).astype(bf16)
    out[...] = jnp.dot(att[...], weight[...], preferred_element_type=f32).astype(bf16)


def add_kernel(tokens, mod, kept, received, out):
    gate = mod[2:3, :]
    step = 64
    for r in range(0, tokens.shape[0], step):
        at = slice(r, r + step)
        mixed = kept[at, :].astype(f32) + received[at, :].astype(f32)
        out[at, :] = (tokens[at, :].astype(f32) + gate * mixed).astype(bf16)


def swapped(array):
    return lax.ppermute(array, "head", [(0, 1), (1, 0)])


def across(array, first):
    count = lax.axis_size("section")
    edges = [(i, i + 1) for i in range(first, count - 1, 2)]
    return lax.ppermute(array, "section", edges + [(j, i) for i, j in edges])


def on_device(
    video_tokens,
    modulation,
    project_weight,
    output_weight,
    norm_gains,
    text_cache,
    text_count,
    video_keep,
    patch_order,
    stale_cache,
):
    sections = lax.axis_size("section")
    place = lax.axis_index("section").astype(jnp.int32).reshape(1)
    side = lax.axis_index("head").astype(jnp.int32).reshape(1)
    rows, model = video_tokens.shape
    size = norm_gains.shape[1]
    width = project_weight.shape[2]
    heads = width // size
    patch = stale_cache.shape[1]
    text_rows = text_cache.shape[1]
    keep = video_keep.reshape(sections, patch)
    half_shape = jax.ShapeDtypeStruct((rows, model), bf16)
    side_shape = jax.ShapeDtypeStruct((patch, width), bf16)
    part_shape = jax.ShapeDtypeStruct((rows, width), bf16)
    total_shape = jax.ShapeDtypeStruct((patch, 2 * width), f32)
    stale_cache = in_hbm(stale_cache)

    normed, to_odd, to_even, values = pl.pallas_call(
        functools.partial(first_kernel, sections),
        out_shape=(half_shape, half_shape, half_shape, side_shape),
        in_specs=[SMEM, HBM, HBM, HBM, HBM],
        out_specs=(HBM,) * 4,
        scratch_shapes=[
            pltpu.SMEM(patch_order.shape, jnp.int32),
            pltpu.VMEM((rows, model), bf16),
            pltpu.VMEM(modulation.shape, f32),
            pltpu.VMEM((patch, width), bf16),
            pltpu.VMEM((patch, width), bf16),
            pltpu.VMEM((rows, model), bf16),
            pltpu.SemaphoreType.DMA((6,)),
            pltpu.SemaphoreType.DMA((8,)),
        ],
        compiler_params=params(10),
        cost_estimate=cost(10 * rows * model, 10 * rows * model),
        name="first",
    )(place, in_hbm(patch_order), in_hbm(video_tokens), in_hbm(modulation), stale_cache)

    odd_own = across(to_odd, 1)
    even_own = across(to_even, 0)
    odd_values = across(values, 1)
    even_values = across(values, 0)
    other = swapped(normed)

    weight_shape = jax.ShapeDtypeStruct((model, width), bf16)
    project_weight = in_hbm(project_weight)
    own_cache, own_keys, key_weight, value_weight = pl.pallas_call(
        own_rows_kernel,
        out_shape=(
            jax.ShapeDtypeStruct((2, rows, width), bf16),
            part_shape,
            weight_shape,
            weight_shape,
        ),
        in_specs=[VMEM, HBM, HBM],
        out_specs=(VMEM,) * 4,
        scratch_shapes=[
            pltpu.VMEM(norm_gains.shape, f32),
            pltpu.SemaphoreType.DMA((3,)),
            pltpu.SemaphoreType.DMA,
        ],
        compiler_params=params(10),
        cost_estimate=cost(4 * rows * model * width, 4 * rows * width),
        name="own_rows",
    )(normed, project_weight, in_hbm(norm_gains))

    fresh_cache, queries, keys, vbuf = pl.pallas_call(
        other_rows_kernel,
        out_shape=(
            jax.ShapeDtypeStruct((2, patch, width), bf16),
            side_shape,
            side_shape,
            jax.ShapeDtypeStruct((heads, patch, 2 * size), bf16),
        ),
        in_specs=[SMEM, SMEM, VMEM, HBM] + [VMEM] * 4 + [HBM, VMEM, VMEM],
        out_specs=(HBM,) + (VMEM,) * 3,
        scratch_shapes=[
            pltpu.VMEM((rows, model), bf16),
            pltpu.VMEM((2, rows, width), bf16),
            pltpu.VMEM((model, width), bf16),
            pltpu.SemaphoreType.DMA((5,)),
        ],
        compiler_params=params(16),
        cost_estimate=cost(8 * rows * model * width, 4 * rows * width),
        name="other_rows",
    )(
        place,
        side,
        normed,
        in_hbm(other),
        own_cache,
        own_keys,
        key_weight,
        value_weight,
        project_weight,
        norm_gains,
        keep,
    )

    total = pl.pallas_call(
        own_kernel,
        out_shape=total_shape,
        in_specs=[SMEM, VMEM, VMEM, VMEM, HBM, VMEM],
        out_specs=VMEM,
        scratch_shapes=[
            pltpu.VMEM((2, text_rows, width), bf16),
            pltpu.VMEM((text_rows, width), bf16),
            pltpu.VMEM((heads, text_rows, 2 * size), bf16),
            pltpu.SemaphoreType.DMA,
        ],
        compiler_params=params(12),
        cost_estimate=cost(6 * patch * (patch + text_rows) * width, 6 * patch * width),
        name="own",
    )(text_count, queries, keys, vbuf, in_hbm(text_cache), norm_gains)

    odd_own, even_own, total = lax.optimization_barrier((odd_own, even_own, total))
    odd_other = swapped(odd_own)
    even_other = swapped(even_own)

    def near(edge, mine, other, total):
        return pl.pallas_call(
            functools.partial(near_kernel, sections, edge),
            out_shape=(total_shape, jax.ShapeDtypeStruct((heads, patch, patch), bf16)),
            in_specs=[SMEM] * 3 + [VMEM] * 8,
            out_specs=(VMEM, VMEM),
            scratch_shapes=[
                pltpu.VMEM((patch, width), bf16),
                pltpu.VMEM((heads, patch, 2 * size), bf16),
            ],
            input_output_aliases={10: 0},
            compiler_params=params(16),
            cost_estimate=cost(4 * patch * model * width, 6 * patch * width),
            name="near_even" if edge else "near_odd",
        )(
            place,
            side,
            patch_order,
            mine,
            other,
            key_weight,
            value_weight,
            norm_gains,
            queries,
            keep,
            total,
        )

    total, odd_weights = near(0, odd_own, odd_other, total)
    total, even_weights = near(1, even_own, even_other, total)

    def finish(flip):
        return pl.pallas_call(
            functools.partial(finish_kernel, sections, flip),
            out_shape=half_shape,
            in_specs=[SMEM] * 3 + [VMEM] * 7,
            out_specs=VMEM,
            scratch_shapes=[
                pltpu.VMEM((heads, patch, 2 * size), bf16),
                pltpu.VMEM((rows, 2 * width), f32),
                pltpu.VMEM((rows, width), bf16),
            ],
            compiler_params=params(20),
            cost_estimate=cost(2 * rows * width * model, 4 * rows * model),
            name="finish_sent" if flip else "finish_kept",
        )(
            place,
            side,
            patch_order,
            odd_weights,
            even_weights,
            odd_values,
            even_values,
            keep,
            total,
            output_weight,
        )

    sent = finish(True)
    received = swapped(sent)
    kept = finish(False)
    updated = pl.pallas_call(
        add_kernel,
        out_shape=half_shape,
        in_specs=[VMEM] * 4,
        out_specs=VMEM,
        compiler_params=params(8),
        cost_estimate=cost(6 * rows * model, 8 * rows * model),
        name="add",
    )(video_tokens, modulation, kept, received)
    return (updated, fresh_cache)


def solution(mesh):
    placed = (
        P(("groups", "section", "head"), None),
        P("groups", None),
        P(None, None, "head"),
        P("head", None),
        P(),
        P(None, "groups", "head"),
        P("groups"),
        P("groups"),
        P("groups"),
        P(None, ("groups", "section"), "head"),
    )

    return jax.shard_map(
        on_device,
        mesh=mesh,
        in_specs=placed,
        out_specs=(P(("groups", "section", "head"), None), P(None, ("groups", "section"), "head")),
        check_vma=False,
    )
```

```python
import functools
import math

import jax
import jax.numpy as jnp
from jax import lax
from jax.experimental import pallas as pl
from jax.experimental.pallas import tpu as pltpu
from jax.sharding import PartitionSpec as P


epsilon = 1e-06
f32 = jnp.float32
bf16 = jnp.bfloat16
MIB = 1024 * 1024

VMEM = pl.BlockSpec(memory_space=pltpu.VMEM)
SMEM = pl.BlockSpec(memory_space=pltpu.SMEM)
HBM = pl.BlockSpec(memory_space=pltpu.HBM)


def params(mib):
    return pltpu.CompilerParams(vmem_limit_bytes=mib * MIB)


def in_hbm(array):
    return pltpu.with_memory_space_constraint(array, pltpu.HBM)


def cost(flops, nbytes):
    return pl.CostEstimate(flops=flops, bytes_accessed=nbytes, transcendentals=0)


def partners(place, sections):
    p = place[0]
    by = 2 * lax.rem(p, 2) - 1
    return tuple(jnp.clip(q, 0, sections - 1) for q in (p + by, p - by))


def gain_row(gains, which):
    return gains[which : which + 1, :]


def head_normed(part, gain):
    spread = jnp.mean(part * part, axis=-1, keepdims=True)
    return (part * lax.rsqrt(spread + epsilon) * gain).astype(bf16)


def heads_normed(part, gain):
    size = gain.shape[-1]
    pieces = [
        head_normed(part[:, i : i + size], gain) for i in range(0, part.shape[-1], size)
    ]
    return jnp.concatenate(pieces, axis=-1)


def mask_columns(row, lanes):
    return jnp.broadcast_to(row, (lanes, row.shape[1])).T.astype(bf16)


def patch_mask(keep, wanted, patch):
    lanes = keep.shape[1]
    count = patch // lanes
    rows = (keep[pl.ds(wanted * count, count), :] > 0).astype(f32)
    return jnp.concatenate(
        [mask_columns(rows[r : r + 1, :], lanes) for r in range(count)], axis=0
    )


def first_kernel(
    sections, place, order_in, x_in, mod_in, stale, normed_out, to_odd, to_even, values_out,
    order, x, mod, held, values, normed, sems, out_sems,
):
    rows, width = x.shape
    part = rows // 2
    half = width // 2
    loads = [(mod_in, mod)] + [(x_in.at[r : r + part], x.at[r : r + part]) for r in (0, part)]
    loads += [(order_in, order), (stale.at[0], held), (stale.at[1], values)]
    copies = [
        pltpu.make_async_copy(source, target, sems.at[i])
        for i, (source, target) in enumerate(loads)
    ]
    for copy in copies:
        copy.start()
    copies[0].wait()
    scale = 1.0 + mod[1:2, :]
    shift = mod[0:1, :]

    def norm(n):
        copies[1 + n].wait()
        step = 64
        for r in range(n * part, (n + 1) * part, step):
            v = x[r : r + step, :].astype(f32)
            shifted = v - jnp.mean(v, axis=-1, keepdims=True)
            spread = jnp.mean(shifted * shifted, axis=-1, keepdims=True)
            y = shifted * lax.rsqrt(spread + epsilon) * scale + shift
            normed[r : r + step, :] = y.astype(bf16)

    norm(0)
    copies[3].wait()
    own = order[place[0]]
    targets = tuple(
        (out, own < order[q]) for out, q in zip((to_odd, to_even), partners(place, sections))
    )
    copies[4].wait()

    def old_copies(n, out):
        return [
            pltpu.make_async_copy(
                held.at[i * rows : (i + 1) * rows],
                out.at[:, i * half : (i + 1) * half],
                out_sems.at[2 * n + i],
            )
            for i in range(2)
        ]

    def new_copy(n, out):
        return pltpu.make_async_copy(normed, out, out_sems.at[4 + n])

    for n, (out, fresh) in enumerate(targets):

        @pl.when(jnp.logical_not(fresh))
        def _():
            for copy in old_copies(n, out):
                copy.start()

    norm(1)
    for n, (out, fresh) in enumerate(targets):

        @pl.when(fresh)
        def _():
            new_copy(n, out).start()

    last = [pltpu.make_async_copy(normed, normed_out, out_sems.at[6])]
    last[0].start()
    copies[5].wait()
    last.append(pltpu.make_async_copy(values, values_out, out_sems.at[7]))
    last[1].start()
    for n, (out, fresh) in enumerate(targets):

        @pl.when(jnp.logical_not(fresh))
        def _():
            for copy in old_copies(n, out):
                copy.wait()

        @pl.when(fresh)
        def _():
            new_copy(n, out).wait()

    for copy in last:
        copy.wait()


def attend(queries, keys, vbuf):
    s = lax.dot_general(queries, keys, (((1,), (1,)), ((), ())), preferred_element_type=f32)
    return jnp.dot(jnp.exp2(s).astype(bf16), vbuf, preferred_element_type=f32)


def own_rows_kernel(
    half, weight, gains_in, cache, keys, key_weight, value_weight, gains, sems, gains_sem
):
    width = keys.shape[1]
    block = 2 * gains.shape[1]
    buffers = {2: value_weight, 1: key_weight}
    pieces = ((2, 0, block), (2, block, width), (1, 0, width))
    copies = []
    for n, (c, low, high) in enumerate(pieces):
        copy = pltpu.make_async_copy(
            weight.at[c, :, low:high], buffers[c].at[:, low:high], sems.at[n]
        )
        copy.start()
        copies.append(copy)
    load_gains = pltpu.make_async_copy(gains_in, gains, gains_sem)
    load_gains.start()
    for n, (c, low, high) in enumerate(pieces):
        copies[n].wait()
        if c == 1:
            load_gains.wait()
            gain = gain_row(gains, 1)
        for j in range(low, high, block):
            cols = slice(j, j + block)
            y = jnp.dot(half[...], buffers[c][:, cols], preferred_element_type=f32)
            y = y.astype(bf16)
            cache[c - 1, :, cols] = y
            if c == 1:
                keys[:, cols] = heads_normed(y.astype(f32), gain)


def other_rows_kernel(
    place, side, own_half, half_in, own_cache, own_keys, key_weight, value_weight, weight, gains,
    keep, cache, queries, keys, vbuf, half, raw, query_weight, sems,
):
    load_half = pltpu.make_async_copy(half_in, half, sems.at[0])
    load_half.start()
    load_weight = pltpu.make_async_copy(weight.at[0], query_weight, sems.at[1])
    rows = half.shape[0]
    width = keys.shape[1]
    size = gains.shape[1]
    block = 2 * size
    h = side[0]
    at = pl.ds(pl.multiple_of((1 - h) * rows, rows), rows)
    own_at = pl.ds(pl.multiple_of(h * rows, rows), rows)
    stores = [
        pltpu.make_async_copy(own_cache, cache.at[:, own_at, :], sems.at[2]),
        pltpu.make_async_copy(raw.at[1], cache.at[1, at, :], sems.at[3]),
        pltpu.make_async_copy(raw.at[0], cache.at[0, at, :], sems.at[4]),
    ]
    mask = patch_mask(keep, place[0], keys.shape[0])
    for i in range(width // size):
        vbuf[i, :, size:] = mask
    keys[own_at, :] = own_keys[...]
    for i in range(width // size):
        vbuf[i, own_at, :size] = (
            own_cache[1, :, i * size : (i + 1) * size] * vbuf[0, own_at, size:]
        )
    gain = gain_row(gains, 1)
    load_half.wait()
    load_weight.start()
    for j in range(0, width, block):
        cols = slice(j, j + block)
        y = jnp.dot(half[...], value_weight[:, cols], preferred_element_type=f32).astype(bf16)
        raw[1, :, cols] = y
        for low in range(0, block, size):
            vbuf[(j + low) // size, at, :size] = y[:, low : low + size] * vbuf[0, at, size:]
    for j in range(0, width, block):
        cols = slice(j, j + block)
        y = jnp.dot(half[...], key_weight[:, cols], preferred_element_type=f32).astype(bf16)
        raw[0, :, cols] = y
        keys[at, cols] = heads_normed(y.astype(f32), gain)
    gain = gain_row(gains, 0) * (math.log2(math.e) * size**-0.5)
    load_weight.wait()
    for store in stores:
        store.start()
    for j in range(0, width, block):
        cols = slice(j, j + block)
        for source, rows_at in ((own_half, own_at), (half, at)):
            y = jnp.dot(source[...], query_weight[:, cols], preferred_element_type=f32)
            queries[rows_at, cols] = heads_normed(y, gain)
    for store in stores:
        store.wait()


def own_kernel(count, queries, keys, vbuf, text_in, gains, total, text, text_keys, tbuf, sem):
    load = pltpu.make_async_copy(text_in, text, sem)
    load.start()
    heads, _, wide = vbuf.shape
    size = wide // 2
    text_rows = text.shape[1]
    for i in range(heads):
        cols = slice(i * size, (i + 1) * size)
        total[:, wide * i : wide * (i + 1)] = attend(queries[:, cols], keys[:, cols], vbuf[i])
    live = lax.broadcasted_iota(jnp.int32, (text_rows, size), 0) < count[0]
    mask = live.astype(f32).astype(bf16)
    gain = gain_row(gains, 2)
    load.wait()
    for i in range(heads):
        cols = slice(i * size, (i + 1) * size)
        text_keys[:, cols] = head_normed(text[0, :, cols].astype(f32), gain)
        tbuf[i, :, :size] = text[1, :, cols] * mask
        tbuf[i, :, size:] = mask
        total[:, wide * i : wide * (i + 1)] += attend(queries[:, cols], text_keys[:, cols], tbuf[i])


def near_kernel(
    sections,
    edge,
    place,
    side,
    order,
    mine,
    other,
    key_weight,
    value_weight,
    gains,
    queries,
    keep,
    total_in,
    total,
    weights,
    keys,
    vbuf,
):
    rows = mine.shape[0]
    patch, width = queries.shape
    size = gains.shape[1]
    block = 2 * size
    heads = width // size
    h = side[0]
    own = order[place[0]]
    q = partners(place, sections)[edge]
    gain = gain_row(gains, 1)
    total[...] = total_in[...]

    @pl.when(order[q] < own)
    def _():
        mask = patch_mask(keep, q, vbuf.shape[1])
        for i in range(heads):
            vbuf[i, :, size:] = mask
        for half, at in ((mine, h), (other, 1 - h)):
            at = pl.ds(pl.multiple_of(at * rows, rows), rows)
            for j in range(0, width, block):
                cols = slice(j, j + block)
                y = jnp.dot(half[...], key_weight[:, cols], preferred_element_type=f32)
                keys[at, cols] = heads_normed(y.astype(bf16).astype(f32), gain)
            for j in range(0, width, block):
                cols = slice(j, j + block)
                y = jnp.dot(half[...], value_weight[:, cols], preferred_element_type=f32)
                y = y.astype(bf16)
                for low in range(0, block, size):
                    vbuf[(j + low) // size, at, :size] = (
                        y[:, low : low + size] * vbuf[0, at, size:]
                    )
        for i in range(heads):
            cols = slice(i * size, (i + 1) * size)
            wide = slice(2 * i * size, 2 * (i + 1) * size)
            total[:, wide] += attend(queries[:, cols], keys[:, cols], vbuf[i])

    @pl.when(order[q] > own)
    def _():
        for r in range(patch // rows):
            keys[r * rows : (r + 1) * rows, :] = heads_normed(
                mine[:, r * width : (r + 1) * width].astype(f32), gain
            )
        for i in range(heads):
            cols = slice(i * size, (i + 1) * size)
            s = lax.dot_general(
                queries[:, cols],
                keys[:, cols],
                (((1,), (1,)), ((), ())),
                preferred_element_type=f32,
            )
            weights[i] = jnp.exp2(s).astype(bf16)


def finish_kernel(
    sections,
    flip,
    place,
    side,
    order,
    odd_weights,
    even_weights,
    odd_values,
    even_values,
    keep,
    total,
    weight,
    out,
    vbuf,
    sums,
    att,
):
    rows = out.shape[0]
    heads = vbuf.shape[0]
    size = vbuf.shape[2] // 2
    h = side[0]
    at = pl.ds(pl.multiple_of((1 - h if flip else h) * rows, rows), rows)
    own = order[place[0]]
    sums[...] = total[at, :]
    odd, even = partners(place, sections)
    for weights, values, q in ((odd_weights, odd_values, odd), (even_weights, even_values, even)):

        @pl.when(order[q] > own)
        def _():
            mask = patch_mask(keep, q, vbuf.shape[1])
            for i in range(heads):
                vbuf[i, :, size:] = mask
                vbuf[i, :, :size] = values[:, i * size : (i + 1) * size] * mask
                sums[:, 2 * i * size : 2 * (i + 1) * size] += jnp.dot(
                    weights[i, at, :], vbuf[i], preferred_element_type=f32
                )

    for i in range(heads):
        low = 2 * i * size
        att[:, i * size : (i + 1) * size] = (
            sums[:, low : low + size] / sums[:, low + size : low + 2 * size]
        ).astype(bf16)
    out[...] = jnp.dot(att[...], weight[...], preferred_element_type=f32).astype(bf16)


def add_kernel(tokens, mod, kept, received, out):
    gate = mod[2:3, :]
    step = 64
    for r in range(0, tokens.shape[0], step):
        at = slice(r, r + step)
        mixed = kept[at, :].astype(f32) + received[at, :].astype(f32)
        out[at, :] = (tokens[at, :].astype(f32) + gate * mixed).astype(bf16)


def swapped(array):
    return lax.ppermute(array, "head", [(0, 1), (1, 0)])


def across(array, first):
    count = lax.axis_size("section")
    edges = [(i, i + 1) for i in range(first, count - 1, 2)]
    return lax.ppermute(array, "section", edges + [(j, i) for i, j in edges])


def on_device(
    video_tokens,
    modulation,
    project_weight,
    output_weight,
    norm_gains,
    text_cache,
    text_count,
    video_keep,
    patch_order,
    stale_cache,
):
    sections = lax.axis_size("section")
    place = lax.axis_index("section").astype(jnp.int32).reshape(1)
    side = lax.axis_index("head").astype(jnp.int32).reshape(1)
    rows, model = video_tokens.shape
    size = norm_gains.shape[1]
    width = project_weight.shape[2]
    heads = width // size
    patch = stale_cache.shape[1]
    text_rows = text_cache.shape[1]
    keep = video_keep.reshape(-1, size)
    half_shape = jax.ShapeDtypeStruct((rows, model), bf16)
    side_shape = jax.ShapeDtypeStruct((patch, width), bf16)
    part_shape = jax.ShapeDtypeStruct((rows, width), bf16)
    total_shape = jax.ShapeDtypeStruct((patch, 2 * width), f32)
    stale_cache = in_hbm(stale_cache)

    normed, to_odd, to_even, values = pl.pallas_call(
        functools.partial(first_kernel, sections),
        out_shape=(half_shape, half_shape, half_shape, side_shape),
        in_specs=[SMEM, HBM, HBM, HBM, HBM],
        out_specs=(HBM,) * 4,
        scratch_shapes=[
            pltpu.SMEM(patch_order.shape, jnp.int32),
            pltpu.VMEM((rows, model), bf16),
            pltpu.VMEM(modulation.shape, f32),
            pltpu.VMEM((patch, width), bf16),
            pltpu.VMEM((patch, width), bf16),
            pltpu.VMEM((rows, model), bf16),
            pltpu.SemaphoreType.DMA((6,)),
            pltpu.SemaphoreType.DMA((8,)),
        ],
        compiler_params=params(10),
        cost_estimate=cost(10 * rows * model, 10 * rows * model),
        name="first",
    )(place, in_hbm(patch_order), in_hbm(video_tokens), in_hbm(modulation), stale_cache)

    odd_own = across(to_odd, 1)
    even_own = across(to_even, 0)
    even_values = across(values, 0)
    odd_values = across(values, 1)
    other = swapped(normed)

    weight_shape = jax.ShapeDtypeStruct((model, width), bf16)
    project_weight = in_hbm(project_weight)
    own_cache, own_keys, key_weight, value_weight = pl.pallas_call(
        own_rows_kernel,
        out_shape=(
            jax.ShapeDtypeStruct((2, rows, width), bf16),
            part_shape,
            weight_shape,
            weight_shape,
        ),
        in_specs=[VMEM, HBM, HBM],
        out_specs=(VMEM,) * 4,
        scratch_shapes=[
            pltpu.VMEM(norm_gains.shape, f32),
            pltpu.SemaphoreType.DMA((3,)),
            pltpu.SemaphoreType.DMA,
        ],
        compiler_params=params(10),
        cost_estimate=cost(4 * rows * model * width, 4 * rows * width),
        name="own_rows",
    )(normed, project_weight, in_hbm(norm_gains))

    fresh_cache, queries, keys, vbuf = pl.pallas_call(
        other_rows_kernel,
        out_shape=(
            jax.ShapeDtypeStruct((2, patch, width), bf16),
            side_shape,
            side_shape,
            jax.ShapeDtypeStruct((heads, patch, 2 * size), bf16),
        ),
        in_specs=[SMEM, SMEM, VMEM, HBM] + [VMEM] * 4 + [HBM, VMEM, VMEM],
        out_specs=(HBM,) + (VMEM,) * 3,
        scratch_shapes=[
            pltpu.VMEM((rows, model), bf16),
            pltpu.VMEM((2, rows, width), bf16),
            pltpu.VMEM((model, width), bf16),
            pltpu.SemaphoreType.DMA((5,)),
        ],
        compiler_params=params(16),
        cost_estimate=cost(8 * rows * model * width, 4 * rows * width),
        name="other_rows",
    )(
        place,
        side,
        normed,
        in_hbm(other),
        own_cache,
        own_keys,
        key_weight,
        value_weight,
        project_weight,
        norm_gains,
        keep,
    )

    odd_own, queries, keys = lax.optimization_barrier((odd_own, queries, keys))
    odd_other = swapped(odd_own)

    total = pl.pallas_call(
        own_kernel,
        out_shape=total_shape,
        in_specs=[SMEM, VMEM, VMEM, VMEM, HBM, VMEM],
        out_specs=VMEM,
        scratch_shapes=[
            pltpu.VMEM((2, text_rows, width), bf16),
            pltpu.VMEM((text_rows, width), bf16),
            pltpu.VMEM((heads, text_rows, 2 * size), bf16),
            pltpu.SemaphoreType.DMA,
        ],
        compiler_params=params(12),
        cost_estimate=cost(6 * patch * (patch + text_rows) * width, 6 * patch * width),
        name="own",
    )(text_count, queries, keys, vbuf, in_hbm(text_cache), norm_gains)

    even_own, total = lax.optimization_barrier((even_own, total))
    even_other = swapped(even_own)

    def near(edge, mine, other, total):
        return pl.pallas_call(
            functools.partial(near_kernel, sections, edge),
            out_shape=(total_shape, jax.ShapeDtypeStruct((heads, patch, patch), bf16)),
            in_specs=[SMEM] * 3 + [VMEM] * 8,
            out_specs=(VMEM, VMEM),
            scratch_shapes=[
                pltpu.VMEM((patch, width), bf16),
                pltpu.VMEM((heads, patch, 2 * size), bf16),
            ],
            input_output_aliases={10: 0},
            compiler_params=params(16),
            cost_estimate=cost(4 * patch * model * width, 6 * patch * width),
            name="near_even" if edge else "near_odd",
        )(
            place,
            side,
            patch_order,
            mine,
            other,
            key_weight,
            value_weight,
            norm_gains,
            queries,
            keep,
            total,
        )

    total, odd_weights = near(0, odd_own, odd_other, total)
    total, even_weights = near(1, even_own, even_other, total)

    def finish(flip):
        return pl.pallas_call(
            functools.partial(finish_kernel, sections, flip),
            out_shape=half_shape,
            in_specs=[SMEM] * 3 + [VMEM] * 7,
            out_specs=VMEM,
            scratch_shapes=[
                pltpu.VMEM((heads, patch, 2 * size), bf16),
                pltpu.VMEM((rows, 2 * width), f32),
                pltpu.VMEM((rows, width), bf16),
            ],
            compiler_params=params(20),
            cost_estimate=cost(2 * rows * width * model, 4 * rows * model),
            name="finish_sent" if flip else "finish_kept",
        )(
            place,
            side,
            patch_order,
            odd_weights,
            even_weights,
            odd_values,
            even_values,
            keep,
            total,
            output_weight,
        )

    sent = finish(True)
    received = swapped(sent)
    kept = finish(False)
    updated = pl.pallas_call(
        add_kernel,
        out_shape=half_shape,
        in_specs=[VMEM] * 4,
        out_specs=VMEM,
        compiler_params=params(8),
        cost_estimate=cost(6 * rows * model, 8 * rows * model),
        name="add",
    )(video_tokens, modulation, kept, received)
    return (updated, fresh_cache)


def solution(mesh):
    placed = (
        P(("groups", "section", "head"), None),
        P("groups", None),
        P(None, None, "head"),
        P("head", None),
        P(),
        P(None, "groups", "head"),
        P("groups"),
        P("groups"),
        P("groups"),
        P(None, ("groups", "section"), "head"),
    )

    return jax.shard_map(
        on_device,
        mesh=mesh,
        in_specs=placed,
        out_specs=(P(("groups", "section", "head"), None), P(None, ("groups", "section"), "head")),
        check_vma=False,
    )
```

```python
import functools
import math

import jax
import jax.numpy as jnp
from jax import lax
from jax.experimental import pallas as pl
from jax.experimental.pallas import tpu as pltpu
from jax.sharding import PartitionSpec as P


epsilon = 1e-06
f32 = jnp.float32
bf16 = jnp.bfloat16
MIB = 1024 * 1024

VMEM = pl.BlockSpec(memory_space=pltpu.VMEM)
SMEM = pl.BlockSpec(memory_space=pltpu.SMEM)
HBM = pl.BlockSpec(memory_space=pltpu.HBM)


def params(mib):
    return pltpu.CompilerParams(vmem_limit_bytes=mib * MIB)


def in_hbm(array):
    return pltpu.with_memory_space_constraint(array, pltpu.HBM)


def cost(flops, nbytes):
    return pl.CostEstimate(flops=flops, bytes_accessed=nbytes, transcendentals=0)


def partners(place, sections):
    p = place[0]
    by = 2 * lax.rem(p, 2) - 1
    return tuple(jnp.clip(q, 0, sections - 1) for q in (p + by, p - by))


def gain_row(gains, which):
    return gains[which : which + 1, :]


def head_normed(part, gain):
    spread = jnp.mean(part * part, axis=-1, keepdims=True)
    return (part * lax.rsqrt(spread + epsilon) * gain).astype(bf16)


def heads_normed(part, gain):
    size = gain.shape[-1]
    pieces = [
        head_normed(part[:, i : i + size], gain) for i in range(0, part.shape[-1], size)
    ]
    return jnp.concatenate(pieces, axis=-1)


def mask_columns(row, lanes):
    return jnp.broadcast_to(row, (lanes, row.shape[1])).T.astype(bf16)


def patch_mask(keep, wanted, patch):
    lanes = keep.shape[1]
    count = patch // lanes
    rows = (keep[pl.ds(wanted * count, count), :] > 0).astype(f32)
    return jnp.concatenate(
        [mask_columns(rows[r : r + 1, :], lanes) for r in range(count)], axis=0
    )


def row_copies(source, target, sems, base, pieces):
    step = source.shape[0] // pieces
    return [
        pltpu.make_async_copy(
            source.at[i * step : (i + 1) * step],
            target.at[i * step : (i + 1) * step],
            sems.at[base + i],
        )
        for i in range(pieces)
    ]


def first_kernel(
    sections, place, order_in, x_in, mod_in, stale, normed_out, to_odd, to_even, values_out,
    order, x, mod, held, values, normed, sems, out_sems,
):
    rows, width = x.shape
    part = rows // 2
    half = width // 2
    loads = [(mod_in, mod)] + [(x_in.at[r : r + part], x.at[r : r + part]) for r in (0, part)]
    loads += [(order_in, order), (stale.at[0], held), (stale.at[1], values)]
    copies = [
        pltpu.make_async_copy(source, target, sems.at[i])
        for i, (source, target) in enumerate(loads)
    ]
    for copy in copies:
        copy.start()
    copies[0].wait()
    scale = 1.0 + mod[1:2, :]
    shift = mod[0:1, :]

    def norm(n):
        copies[1 + n].wait()
        step = 64
        for r in range(n * part, (n + 1) * part, step):
            v = x[r : r + step, :].astype(f32)
            shifted = v - jnp.mean(v, axis=-1, keepdims=True)
            spread = jnp.mean(shifted * shifted, axis=-1, keepdims=True)
            y = shifted * lax.rsqrt(spread + epsilon) * scale + shift
            normed[r : r + step, :] = y.astype(bf16)

    norm(0)
    copies[3].wait()
    own = order[place[0]]
    targets = tuple(
        (out, own < order[q]) for out, q in zip((to_odd, to_even), partners(place, sections))
    )
    copies[4].wait()

    def old_copies(n, out):
        return [
            pltpu.make_async_copy(
                held.at[i * rows : (i + 1) * rows],
                out.at[:, i * half : (i + 1) * half],
                out_sems.at[2 * n + i],
            )
            for i in range(2)
        ]

    def new_copy(n, out):
        return pltpu.make_async_copy(normed, out, out_sems.at[4 + n])

    for n, (out, fresh) in enumerate(targets):

        @pl.when(jnp.logical_not(fresh))
        def _():
            for copy in old_copies(n, out):
                copy.start()

    norm(1)
    for n, (out, fresh) in enumerate(targets):

        @pl.when(fresh)
        def _():
            new_copy(n, out).start()

    last = [pltpu.make_async_copy(normed, normed_out, out_sems.at[6])]
    last[0].start()
    copies[5].wait()
    last.append(pltpu.make_async_copy(values, values_out, out_sems.at[7]))
    last[1].start()
    for n, (out, fresh) in enumerate(targets):

        @pl.when(jnp.logical_not(fresh))
        def _():
            for copy in old_copies(n, out):
                copy.wait()

        @pl.when(fresh)
        def _():
            new_copy(n, out).wait()

    for copy in last:
        copy.wait()


def attend(queries, keys, vbuf):
    s = lax.dot_general(queries, keys, (((1,), (1,)), ((), ())), preferred_element_type=f32)
    return jnp.dot(jnp.exp2(s).astype(bf16), vbuf, preferred_element_type=f32)


def own_rows_kernel(
    half, weight, gains_in, cache, keys, key_weight, value_weight, gains, sems, gains_sem
):
    width = keys.shape[1]
    block = 2 * gains.shape[1]
    buffers = {2: value_weight, 1: key_weight}
    pieces = [(c, low, low + block) for c in (2, 1) for low in range(0, width, block)]
    copies = [
        pltpu.make_async_copy(
            weight.at[c, :, low:high], buffers[c].at[:, low:high], sems.at[n]
        )
        for n, (c, low, high) in enumerate(pieces)
    ]
    for copy in copies:
        copy.start()
    load_gains = pltpu.make_async_copy(gains_in, gains, gains_sem)
    load_gains.start()
    waits = {0: copies[:1], 1: copies[1 : width // block], width // block: copies[width // block :]}
    for n, (c, low, high) in enumerate(pieces):
        for copy in waits.get(n, ()):
            copy.wait()
        if n == width // block:
            load_gains.wait()
            gain = gain_row(gains, 1)
        cols = slice(low, high)
        y = jnp.dot(half[...], buffers[c][:, cols], preferred_element_type=f32).astype(bf16)
        cache[c - 1, :, cols] = y
        if c == 1:
            keys[:, cols] = heads_normed(y.astype(f32), gain)


def other_rows_kernel(
    place, side, own_half, half_in, own_cache, own_keys, key_weight, value_weight, weight, gains,
    keep, cache, queries, keys, vbuf, half, raw, query_weight, sems,
):
    load_half = row_copies(half_in, half, sems, 0, 2)
    load_weight = row_copies(weight.at[0], query_weight, sems, 2, 6)
    for copy in load_half + load_weight:
        copy.start()
    rows = half.shape[0]
    width = keys.shape[1]
    size = gains.shape[1]
    block = 2 * size
    h = side[0]
    at = pl.ds(pl.multiple_of((1 - h) * rows, rows), rows)
    own_at = pl.ds(pl.multiple_of(h * rows, rows), rows)
    stores = [
        pltpu.make_async_copy(own_cache.at[0], cache.at[0, own_at, :], sems.at[8]),
        pltpu.make_async_copy(own_cache.at[1], cache.at[1, own_at, :], sems.at[9]),
        pltpu.make_async_copy(raw.at[0], cache.at[0, at, :], sems.at[10]),
        pltpu.make_async_copy(raw.at[1], cache.at[1, at, :], sems.at[11]),
    ]
    mask = patch_mask(keep, place[0], keys.shape[0])
    for i in range(width // size):
        vbuf[i, :, size:] = mask
    keys[own_at, :] = own_keys[...]
    for i in range(width // size):
        vbuf[i, own_at, :size] = (
            own_cache[1, :, i * size : (i + 1) * size] * vbuf[0, own_at, size:]
        )
    gain = gain_row(gains, 1)
    for copy in load_half:
        copy.wait()
    for j in range(0, width, block):
        cols = slice(j, j + block)
        y = jnp.dot(half[...], value_weight[:, cols], preferred_element_type=f32).astype(bf16)
        raw[1, :, cols] = y
        for low in range(0, block, size):
            vbuf[(j + low) // size, at, :size] = y[:, low : low + size] * vbuf[0, at, size:]
    for j in range(0, width, block):
        cols = slice(j, j + block)
        y = jnp.dot(half[...], key_weight[:, cols], preferred_element_type=f32).astype(bf16)
        raw[0, :, cols] = y
        keys[at, cols] = heads_normed(y.astype(f32), gain)
    gain = gain_row(gains, 0) * (math.log2(math.e) * size**-0.5)
    for copy in load_weight:
        copy.wait()
    for store in stores:
        store.start()
    for j in range(0, width, block):
        cols = slice(j, j + block)
        for source, rows_at in ((own_half, own_at), (half, at)):
            y = jnp.dot(source[...], query_weight[:, cols], preferred_element_type=f32)
            queries[rows_at, cols] = heads_normed(y, gain)
    for store in stores:
        store.wait()


def own_kernel(count, queries, keys, vbuf, text_in, gains, total, text, text_keys, tbuf, sem):
    load = pltpu.make_async_copy(text_in, text, sem)
    load.start()
    heads, _, wide = vbuf.shape
    size = wide // 2
    text_rows = text.shape[1]
    for i in range(heads):
        cols = slice(i * size, (i + 1) * size)
        total[:, wide * i : wide * (i + 1)] = attend(queries[:, cols], keys[:, cols], vbuf[i])
    live = lax.broadcasted_iota(jnp.int32, (text_rows, size), 0) < count[0]
    mask = live.astype(f32).astype(bf16)
    gain = gain_row(gains, 2)
    load.wait()
    for i in range(heads):
        cols = slice(i * size, (i + 1) * size)
        text_keys[:, cols] = head_normed(text[0, :, cols].astype(f32), gain)
        tbuf[i, :, :size] = text[1, :, cols] * mask
        tbuf[i, :, size:] = mask
        total[:, wide * i : wide * (i + 1)] += attend(queries[:, cols], text_keys[:, cols], tbuf[i])


def near_kernel(
    sections,
    edge,
    place,
    side,
    order,
    mine_in,
    other,
    key_weight,
    value_weight,
    gains,
    queries,
    keep,
    total_in,
    total,
    weights,
    keys,
    vbuf,
    *buffers,
):
    loads = []
    mine = mine_in
    if buffers:
        mine, sems = buffers
        loads = row_copies(mine_in, mine, sems, 0, 2)
    for copy in loads:
        copy.start()
    rows = mine.shape[0]
    patch, width = queries.shape
    size = gains.shape[1]
    block = 2 * size
    heads = width // size
    h = side[0]
    own = order[place[0]]
    q = partners(place, sections)[edge]
    gain = gain_row(gains, 1)
    fresh = order[q] < own

    @pl.when(jnp.logical_not(fresh))
    def _():
        total[...] = total_in[...]
        for copy in loads:
            copy.wait()

    @pl.when(fresh)
    def _():
        mask = patch_mask(keep, q, vbuf.shape[1])
        for i in range(heads):
            vbuf[i, :, size:] = mask
        for half, at in ((other, 1 - h), (mine, h)):
            if half is mine:
                for copy in loads:
                    copy.wait()
            at = pl.ds(pl.multiple_of(at * rows, rows), rows)
            for j in range(0, width, block):
                cols = slice(j, j + block)
                y = jnp.dot(half[...], key_weight[:, cols], preferred_element_type=f32)
                keys[at, cols] = heads_normed(y.astype(bf16).astype(f32), gain)
            for j in range(0, width, block):
                cols = slice(j, j + block)
                y = jnp.dot(half[...], value_weight[:, cols], preferred_element_type=f32)
                y = y.astype(bf16)
                for low in range(0, block, size):
                    vbuf[(j + low) // size, at, :size] = (
                        y[:, low : low + size] * vbuf[0, at, size:]
                    )
        for i in range(heads):
            cols = slice(i * size, (i + 1) * size)
            wide = slice(2 * i * size, 2 * (i + 1) * size)
            total[:, wide] = total_in[:, wide] + attend(queries[:, cols], keys[:, cols], vbuf[i])

    @pl.when(order[q] > own)
    def _():
        for r in range(patch // rows):
            keys[r * rows : (r + 1) * rows, :] = heads_normed(
                mine[:, r * width : (r + 1) * width].astype(f32), gain
            )
        for i in range(heads):
            cols = slice(i * size, (i + 1) * size)
            s = lax.dot_general(
                queries[:, cols],
                keys[:, cols],
                (((1,), (1,)), ((), ())),
                preferred_element_type=f32,
            )
            weights[i] = jnp.exp2(s).astype(bf16)


def finish_kernel(
    sections,
    flip,
    place,
    side,
    order,
    odd_weights,
    even_weights,
    odd_values,
    even_values,
    keep,
    total,
    weight,
    out,
    vbuf,
    sums,
    att,
):
    rows = out.shape[0]
    heads = vbuf.shape[0]
    size = vbuf.shape[2] // 2
    h = side[0]
    at = pl.ds(pl.multiple_of((1 - h if flip else h) * rows, rows), rows)
    own = order[place[0]]
    sums[...] = total[at, :]
    odd, even = partners(place, sections)
    for weights, values, q in ((odd_weights, odd_values, odd), (even_weights, even_values, even)):

        @pl.when(order[q] > own)
        def _():
            mask = patch_mask(keep, q, vbuf.shape[1])
            for i in range(heads):
                vbuf[i, :, size:] = mask
                vbuf[i, :, :size] = values[:, i * size : (i + 1) * size] * mask
                sums[:, 2 * i * size : 2 * (i + 1) * size] += jnp.dot(
                    weights[i, at, :], vbuf[i], preferred_element_type=f32
                )

    for i in range(heads):
        low = 2 * i * size
        att[:, i * size : (i + 1) * size] = (
            sums[:, low : low + size] / sums[:, low + size : low + 2 * size]
        ).astype(bf16)
    out[...] = jnp.dot(att[...], weight[...], preferred_element_type=f32).astype(bf16)


def add_kernel(tokens, mod, kept, received, out, held, sems):
    gate = mod[2:3, :]
    copies = row_copies(held, out, sems, 0, 4)
    step = held.shape[0] // len(copies)
    for n, copy in enumerate(copies):
        at = slice(n * step, (n + 1) * step)
        mixed = kept[at, :].astype(f32) + received[at, :].astype(f32)
        held[at, :] = (tokens[at, :].astype(f32) + gate * mixed).astype(bf16)
        copy.start()
    for copy in copies:
        copy.wait()


def swapped(array):
    return lax.ppermute(array, "head", [(0, 1), (1, 0)])


def across(array, first):
    count = lax.axis_size("section")
    edges = [(i, i + 1) for i in range(first, count - 1, 2)]
    return lax.ppermute(array, "section", edges + [(j, i) for i, j in edges])


def on_device(
    video_tokens,
    modulation,
    project_weight,
    output_weight,
    norm_gains,
    text_cache,
    text_count,
    video_keep,
    patch_order,
    stale_cache,
):
    sections = lax.axis_size("section")
    place = lax.axis_index("section").astype(jnp.int32).reshape(1)
    side = lax.axis_index("head").astype(jnp.int32).reshape(1)
    rows, model = video_tokens.shape
    size = norm_gains.shape[1]
    width = project_weight.shape[2]
    heads = width // size
    patch = stale_cache.shape[1]
    text_rows = text_cache.shape[1]
    keep = video_keep.reshape(-1, size)
    half_shape = jax.ShapeDtypeStruct((rows, model), bf16)
    side_shape = jax.ShapeDtypeStruct((patch, width), bf16)
    part_shape = jax.ShapeDtypeStruct((rows, width), bf16)
    total_shape = jax.ShapeDtypeStruct((patch, 2 * width), f32)
    stale_cache = in_hbm(stale_cache)

    normed, to_odd, to_even, values = pl.pallas_call(
        functools.partial(first_kernel, sections),
        out_shape=(half_shape, half_shape, half_shape, side_shape),
        in_specs=[SMEM, HBM, HBM, HBM, HBM],
        out_specs=(HBM,) * 4,
        scratch_shapes=[
            pltpu.SMEM(patch_order.shape, jnp.int32),
            pltpu.VMEM((rows, model), bf16),
            pltpu.VMEM(modulation.shape, f32),
            pltpu.VMEM((patch, width), bf16),
            pltpu.VMEM((patch, width), bf16),
            pltpu.VMEM((rows, model), bf16),
            pltpu.SemaphoreType.DMA((6,)),
            pltpu.SemaphoreType.DMA((8,)),
        ],
        compiler_params=params(10),
        cost_estimate=cost(10 * rows * model, 10 * rows * model),
        name="first",
    )(place, in_hbm(patch_order), in_hbm(video_tokens), in_hbm(modulation), stale_cache)

    odd_own = across(to_odd, 1)
    even_own = across(to_even, 0)
    even_values = across(values, 0)
    odd_values = across(values, 1)
    other = swapped(normed)

    weight_shape = jax.ShapeDtypeStruct((model, width), bf16)
    project_weight = in_hbm(project_weight)
    own_cache, own_keys, key_weight, value_weight = pl.pallas_call(
        own_rows_kernel,
        out_shape=(
            jax.ShapeDtypeStruct((2, rows, width), bf16),
            part_shape,
            weight_shape,
            weight_shape,
        ),
        in_specs=[VMEM, HBM, HBM],
        out_specs=(VMEM,) * 4,
        scratch_shapes=[
            pltpu.VMEM(norm_gains.shape, f32),
            pltpu.SemaphoreType.DMA((width // size,)),
            pltpu.SemaphoreType.DMA,
        ],
        compiler_params=params(10),
        cost_estimate=cost(4 * rows * model * width, 4 * rows * width),
        name="own_rows",
    )(normed, project_weight, in_hbm(norm_gains))

    fresh_cache, queries, keys, vbuf = pl.pallas_call(
        other_rows_kernel,
        out_shape=(
            jax.ShapeDtypeStruct((2, patch, width), bf16),
            side_shape,
            side_shape,
            jax.ShapeDtypeStruct((heads, patch, 2 * size), bf16),
        ),
        in_specs=[SMEM, SMEM, VMEM, HBM] + [VMEM] * 4 + [HBM, VMEM, VMEM],
        out_specs=(HBM,) + (VMEM,) * 3,
        scratch_shapes=[
            pltpu.VMEM((rows, model), bf16),
            pltpu.VMEM((2, rows, width), bf16),
            pltpu.VMEM((model, width), bf16),
            pltpu.SemaphoreType.DMA((12,)),
        ],
        compiler_params=params(16),
        cost_estimate=cost(8 * rows * model * width, 4 * rows * width),
        name="other_rows",
    )(
        place,
        side,
        normed,
        in_hbm(other),
        own_cache,
        own_keys,
        key_weight,
        value_weight,
        project_weight,
        norm_gains,
        keep,
    )

    odd_own, queries, keys = lax.optimization_barrier((odd_own, queries, keys))
    odd_other = swapped(odd_own)

    total = pl.pallas_call(
        own_kernel,
        out_shape=total_shape,
        in_specs=[SMEM, VMEM, VMEM, VMEM, HBM, VMEM],
        out_specs=VMEM,
        scratch_shapes=[
            pltpu.VMEM((2, text_rows, width), bf16),
            pltpu.VMEM((text_rows, width), bf16),
            pltpu.VMEM((heads, text_rows, 2 * size), bf16),
            pltpu.SemaphoreType.DMA,
        ],
        compiler_params=params(12),
        cost_estimate=cost(6 * patch * (patch + text_rows) * width, 6 * patch * width),
        name="own",
    )(text_count, queries, keys, vbuf, in_hbm(text_cache), norm_gains)

    even_own, total = lax.optimization_barrier((even_own, total))
    even_other = swapped(even_own)

    def near(edge, mine, other, total):
        buffers = []
        if edge == 0:
            mine = in_hbm(mine)
            buffers = [pltpu.VMEM((rows, model), bf16), pltpu.SemaphoreType.DMA((2,))]
        return pl.pallas_call(
            functools.partial(near_kernel, sections, edge),
            out_shape=(total_shape, jax.ShapeDtypeStruct((heads, patch, patch), bf16)),
            in_specs=[SMEM] * 3 + [VMEM if edge else HBM] + [VMEM] * 7,
            out_specs=(VMEM, VMEM),
            scratch_shapes=[
                pltpu.VMEM((patch, width), bf16),
                pltpu.VMEM((heads, patch, 2 * size), bf16),
            ]
            + buffers,
            input_output_aliases={10: 0},
            compiler_params=params(16),
            cost_estimate=cost(4 * patch * model * width, 6 * patch * width),
            name="near_even" if edge else "near_odd",
        )(
            place,
            side,
            patch_order,
            mine,
            other,
            key_weight,
            value_weight,
            norm_gains,
            queries,
            keep,
            total,
        )

    total, odd_weights = near(0, odd_own, odd_other, total)
    total, even_weights = near(1, even_own, even_other, total)

    def finish(flip):
        return pl.pallas_call(
            functools.partial(finish_kernel, sections, flip),
            out_shape=half_shape,
            in_specs=[SMEM] * 3 + [VMEM] * 7,
            out_specs=VMEM,
            scratch_shapes=[
                pltpu.VMEM((heads, patch, 2 * size), bf16),
                pltpu.VMEM((rows, 2 * width), f32),
                pltpu.VMEM((rows, width), bf16),
            ],
            compiler_params=params(20),
            cost_estimate=cost(2 * rows * width * model, 4 * rows * model),
            name="finish_sent" if flip else "finish_kept",
        )(
            place,
            side,
            patch_order,
            odd_weights,
            even_weights,
            odd_values,
            even_values,
            keep,
            total,
            output_weight,
        )

    sent = finish(True)
    received = swapped(sent)
    kept = finish(False)
    updated = pl.pallas_call(
        add_kernel,
        out_shape=half_shape,
        in_specs=[VMEM] * 4,
        out_specs=HBM,
        scratch_shapes=[pltpu.VMEM((rows, model), bf16), pltpu.SemaphoreType.DMA((4,))],
        compiler_params=params(8),
        cost_estimate=cost(6 * rows * model, 8 * rows * model),
        name="add",
    )(video_tokens, modulation, kept, received)
    return (updated, fresh_cache)


def solution(mesh):
    placed = (
        P(("groups", "section", "head"), None),
        P("groups", None),
        P(None, None, "head"),
        P("head", None),
        P(),
        P(None, "groups", "head"),
        P("groups"),
        P("groups"),
        P("groups"),
        P(None, ("groups", "section"), "head"),
    )

    return jax.shard_map(
        on_device,
        mesh=mesh,
        in_specs=placed,
        out_specs=(P(("groups", "section", "head"), None), P(None, ("groups", "section"), "head")),
        check_vma=False,
    )
```

```python
import functools
import math

import jax
import jax.numpy as jnp
from jax import lax
from jax.experimental import pallas as pl
from jax.experimental.pallas import tpu as pltpu
from jax.sharding import PartitionSpec as P


epsilon = 1e-06
f32 = jnp.float32
bf16 = jnp.bfloat16
MIB = 1024 * 1024

VMEM = pl.BlockSpec(memory_space=pltpu.VMEM)
SMEM = pl.BlockSpec(memory_space=pltpu.SMEM)
HBM = pl.BlockSpec(memory_space=pltpu.HBM)


def params(mib):
    return pltpu.CompilerParams(vmem_limit_bytes=mib * MIB)


def in_hbm(array):
    return pltpu.with_memory_space_constraint(array, pltpu.HBM)


def cost(flops, nbytes):
    return pl.CostEstimate(flops=flops, bytes_accessed=nbytes, transcendentals=0)


def partners(place, sections):
    p = place[0]
    by = 2 * lax.rem(p, 2) - 1
    return tuple(jnp.clip(q, 0, sections - 1) for q in (p + by, p - by))


def gain_row(gains, which):
    return gains[which : which + 1, :]


def head_normed(part, gain):
    spread = jnp.mean(part * part, axis=-1, keepdims=True)
    return (part * lax.rsqrt(spread + epsilon) * gain).astype(bf16)


def heads_normed(part, gain):
    size = gain.shape[-1]
    pieces = [
        head_normed(part[:, i : i + size], gain) for i in range(0, part.shape[-1], size)
    ]
    return jnp.concatenate(pieces, axis=-1)


def mask_columns(row, lanes):
    return jnp.broadcast_to(row, (lanes, row.shape[1])).T.astype(bf16)


def patch_mask(keep, wanted, patch):
    lanes = keep.shape[1]
    count = patch // lanes
    rows = (keep[pl.ds(wanted * count, count), :] > 0).astype(f32)
    return jnp.concatenate(
        [mask_columns(rows[r : r + 1, :], lanes) for r in range(count)], axis=0
    )


def row_copies(source, target, sems, base, pieces):
    step = source.shape[0] // pieces
    return [
        pltpu.make_async_copy(
            source.at[i * step : (i + 1) * step],
            target.at[i * step : (i + 1) * step],
            sems.at[base + i],
        )
        for i in range(pieces)
    ]


def first_kernel(
    sections, place, order_in, x_in, mod_in, stale, normed_out, to_odd, to_even, values_out,
    order, x, mod, held, values, normed, sems, out_sems,
):
    rows, width = x.shape
    part = rows // 2
    half = width // 2
    loads = [(mod_in, mod)] + [(x_in.at[r : r + part], x.at[r : r + part]) for r in (0, part)]
    loads += [(order_in, order), (stale.at[0], held), (stale.at[1], values)]
    copies = [
        pltpu.make_async_copy(source, target, sems.at[i])
        for i, (source, target) in enumerate(loads)
    ]
    for copy in copies:
        copy.start()
    copies[0].wait()
    scale = 1.0 + mod[1:2, :]
    shift = mod[0:1, :]

    def norm(n):
        copies[1 + n].wait()
        step = 64
        for r in range(n * part, (n + 1) * part, step):
            v = x[r : r + step, :].astype(f32)
            shifted = v - jnp.mean(v, axis=-1, keepdims=True)
            spread = jnp.mean(shifted * shifted, axis=-1, keepdims=True)
            y = shifted * lax.rsqrt(spread + epsilon) * scale + shift
            normed[r : r + step, :] = y.astype(bf16)

    norm(0)
    copies[3].wait()
    own = order[place[0]]
    targets = tuple(
        (out, own < order[q]) for out, q in zip((to_odd, to_even), partners(place, sections))
    )
    copies[4].wait()

    def old_copies(n, out):
        return [
            pltpu.make_async_copy(
                held.at[i * rows : (i + 1) * rows],
                out.at[:, i * half : (i + 1) * half],
                out_sems.at[2 * n + i],
            )
            for i in range(2)
        ]

    def new_copy(n, out):
        return pltpu.make_async_copy(normed, out, out_sems.at[4 + n])

    for n, (out, fresh) in enumerate(targets):

        @pl.when(jnp.logical_not(fresh))
        def _():
            for copy in old_copies(n, out):
                copy.start()

    norm(1)
    for n, (out, fresh) in enumerate(targets):

        @pl.when(fresh)
        def _():
            new_copy(n, out).start()

    last = [pltpu.make_async_copy(normed, normed_out, out_sems.at[6])]
    last[0].start()
    copies[5].wait()
    last.append(pltpu.make_async_copy(values, values_out, out_sems.at[7]))
    last[1].start()
    for n, (out, fresh) in enumerate(targets):

        @pl.when(jnp.logical_not(fresh))
        def _():
            for copy in old_copies(n, out):
                copy.wait()

        @pl.when(fresh)
        def _():
            new_copy(n, out).wait()

    for copy in last:
        copy.wait()


def attend(queries, keys, vbuf):
    s = lax.dot_general(queries, keys, (((1,), (1,)), ((), ())), preferred_element_type=f32)
    return jnp.dot(jnp.exp2(s).astype(bf16), vbuf, preferred_element_type=f32)


def own_rows_kernel(
    half, weight, gains_in, cache, keys, key_weight, value_weight, gains, sems, gains_sem
):
    width = keys.shape[1]
    block = 2 * gains.shape[1]
    buffers = {2: value_weight, 1: key_weight}
    pieces = [(c, low, low + block) for c in (2, 1) for low in range(0, width, block)]
    copies = [
        pltpu.make_async_copy(
            weight.at[c, :, low:high], buffers[c].at[:, low:high], sems.at[n]
        )
        for n, (c, low, high) in enumerate(pieces)
    ]
    for copy in copies:
        copy.start()
    load_gains = pltpu.make_async_copy(gains_in, gains, gains_sem)
    load_gains.start()
    waits = {0: copies[:1], 1: copies[1 : width // block], width // block: copies[width // block :]}
    for n, (c, low, high) in enumerate(pieces):
        for copy in waits.get(n, ()):
            copy.wait()
        if n == width // block:
            load_gains.wait()
            gain = gain_row(gains, 1)
        cols = slice(low, high)
        y = jnp.dot(half[...], buffers[c][:, cols], preferred_element_type=f32).astype(bf16)
        cache[c - 1, :, cols] = y
        if c == 1:
            keys[:, cols] = heads_normed(y.astype(f32), gain)


def other_rows_kernel(
    place, side, own_half, half_in, own_cache, own_keys, key_weight, value_weight, weight, gains,
    keep, cache, queries, keys, vbuf, half, raw, query_weight, sems,
):
    load_half = row_copies(half_in, half, sems, 0, 2)
    load_weight = row_copies(weight.at[0], query_weight, sems, 2, 6)
    for copy in load_half + load_weight:
        copy.start()
    rows = half.shape[0]
    width = keys.shape[1]
    size = gains.shape[1]
    block = 2 * size
    h = side[0]
    at = pl.ds(pl.multiple_of((1 - h) * rows, rows), rows)
    own_at = pl.ds(pl.multiple_of(h * rows, rows), rows)
    stores = [
        pltpu.make_async_copy(own_cache.at[0], cache.at[0, own_at, :], sems.at[8]),
        pltpu.make_async_copy(own_cache.at[1], cache.at[1, own_at, :], sems.at[9]),
        pltpu.make_async_copy(raw.at[0], cache.at[0, at, :], sems.at[10]),
        pltpu.make_async_copy(raw.at[1], cache.at[1, at, :], sems.at[11]),
    ]
    mask = patch_mask(keep, place[0], keys.shape[0])
    for i in range(width // size):
        vbuf[i, :, size:] = mask
    keys[own_at, :] = own_keys[...]
    for i in range(width // size):
        vbuf[i, own_at, :size] = (
            own_cache[1, :, i * size : (i + 1) * size] * vbuf[0, own_at, size:]
        )
    gain = gain_row(gains, 1)
    for copy in load_half:
        copy.wait()
    stores[0].start()
    stores[1].start()
    for j in range(0, width, block):
        cols = slice(j, j + block)
        y = jnp.dot(half[...], value_weight[:, cols], preferred_element_type=f32).astype(bf16)
        raw[1, :, cols] = y
        for low in range(0, block, size):
            vbuf[(j + low) // size, at, :size] = y[:, low : low + size] * vbuf[0, at, size:]
    for j in range(0, width, block):
        cols = slice(j, j + block)
        y = jnp.dot(half[...], key_weight[:, cols], preferred_element_type=f32).astype(bf16)
        raw[0, :, cols] = y
        keys[at, cols] = heads_normed(y.astype(f32), gain)
    gain = gain_row(gains, 0) * (math.log2(math.e) * size**-0.5)
    stores[2].start()
    stores[3].start()
    for copy in load_weight:
        copy.wait()
    for j in range(0, width, block):
        cols = slice(j, j + block)
        for source, rows_at in ((own_half, own_at), (half, at)):
            y = jnp.dot(source[...], query_weight[:, cols], preferred_element_type=f32)
            queries[rows_at, cols] = heads_normed(y, gain)
    for store in stores:
        store.wait()


def own_kernel(count, queries, keys, vbuf, text_in, gains, total, text, text_keys, tbuf, sem):
    load = pltpu.make_async_copy(text_in, text, sem)
    load.start()
    heads, _, wide = vbuf.shape
    size = wide // 2
    text_rows = text.shape[1]
    for i in range(heads):
        cols = slice(i * size, (i + 1) * size)
        total[:, wide * i : wide * (i + 1)] = attend(queries[:, cols], keys[:, cols], vbuf[i])
    live = lax.broadcasted_iota(jnp.int32, (text_rows, size), 0) < count[0]
    mask = live.astype(f32).astype(bf16)
    gain = gain_row(gains, 2)
    load.wait()
    for i in range(heads):
        cols = slice(i * size, (i + 1) * size)
        text_keys[:, cols] = head_normed(text[0, :, cols].astype(f32), gain)
        tbuf[i, :, :size] = text[1, :, cols] * mask
        tbuf[i, :, size:] = mask
        total[:, wide * i : wide * (i + 1)] += attend(queries[:, cols], text_keys[:, cols], tbuf[i])


def near_kernel(
    sections,
    edge,
    place,
    side,
    order,
    mine_in,
    other,
    key_weight,
    value_weight,
    gains,
    queries,
    keep,
    total_in,
    total,
    weights,
    keys,
    vbuf,
    *buffers,
):
    loads = []
    mine = mine_in
    if buffers:
        mine, sems = buffers
        loads = row_copies(mine_in, mine, sems, 0, 2)
    for copy in loads:
        copy.start()
    rows = mine.shape[0]
    patch, width = queries.shape
    size = gains.shape[1]
    block = 2 * size
    heads = width // size
    h = side[0]
    own = order[place[0]]
    q = partners(place, sections)[edge]
    gain = gain_row(gains, 1)
    fresh = order[q] < own

    @pl.when(jnp.logical_not(fresh))
    def _():
        total[...] = total_in[...]
        for copy in loads:
            copy.wait()

    @pl.when(fresh)
    def _():
        mask = patch_mask(keep, q, vbuf.shape[1])
        for i in range(heads):
            vbuf[i, :, size:] = mask
        for half, at in ((other, 1 - h), (mine, h)):
            if half is mine:
                for copy in loads:
                    copy.wait()
            at = pl.ds(pl.multiple_of(at * rows, rows), rows)
            for j in range(0, width, block):
                cols = slice(j, j + block)
                y = jnp.dot(half[...], key_weight[:, cols], preferred_element_type=f32)
                keys[at, cols] = heads_normed(y.astype(bf16).astype(f32), gain)
            for j in range(0, width, block):
                cols = slice(j, j + block)
                y = jnp.dot(half[...], value_weight[:, cols], preferred_element_type=f32)
                y = y.astype(bf16)
                for low in range(0, block, size):
                    vbuf[(j + low) // size, at, :size] = (
                        y[:, low : low + size] * vbuf[0, at, size:]
                    )
        for i in range(heads):
            cols = slice(i * size, (i + 1) * size)
            wide = slice(2 * i * size, 2 * (i + 1) * size)
            total[:, wide] = total_in[:, wide] + attend(queries[:, cols], keys[:, cols], vbuf[i])

    @pl.when(order[q] > own)
    def _():
        for r in range(patch // rows):
            keys[r * rows : (r + 1) * rows, :] = heads_normed(
                mine[:, r * width : (r + 1) * width].astype(f32), gain
            )
        for i in range(heads):
            cols = slice(i * size, (i + 1) * size)
            s = lax.dot_general(
                queries[:, cols],
                keys[:, cols],
                (((1,), (1,)), ((), ())),
                preferred_element_type=f32,
            )
            weights[i] = jnp.exp2(s).astype(bf16)


def finish_kernel(
    sections,
    flip,
    place,
    side,
    order,
    odd_weights,
    even_weights,
    odd_values,
    even_values,
    keep,
    total,
    weight,
    out,
    vbuf,
    sums,
    att,
):
    rows = out.shape[0]
    heads = vbuf.shape[0]
    size = vbuf.shape[2] // 2
    h = side[0]
    at = pl.ds(pl.multiple_of((1 - h if flip else h) * rows, rows), rows)
    own = order[place[0]]
    sums[...] = total[at, :]
    odd, even = partners(place, sections)
    for weights, values, q in ((odd_weights, odd_values, odd), (even_weights, even_values, even)):

        @pl.when(order[q] > own)
        def _():
            mask = patch_mask(keep, q, vbuf.shape[1])
            for i in range(heads):
                vbuf[i, :, size:] = mask
                vbuf[i, :, :size] = values[:, i * size : (i + 1) * size] * mask
                sums[:, 2 * i * size : 2 * (i + 1) * size] += jnp.dot(
                    weights[i, at, :], vbuf[i], preferred_element_type=f32
                )

    for i in range(heads):
        low = 2 * i * size
        att[:, i * size : (i + 1) * size] = (
            sums[:, low : low + size] / sums[:, low + size : low + 2 * size]
        ).astype(bf16)
    out[...] = jnp.dot(att[...], weight[...], preferred_element_type=f32).astype(bf16)


def add_kernel(tokens, mod, kept, received, out, held, sems):
    gate = mod[2:3, :]
    copies = row_copies(held, out, sems, 0, 4)
    step = held.shape[0] // len(copies)
    for n, copy in enumerate(copies):
        at = slice(n * step, (n + 1) * step)
        mixed = kept[at, :].astype(f32) + received[at, :].astype(f32)
        held[at, :] = (tokens[at, :].astype(f32) + gate * mixed).astype(bf16)
        copy.start()
    for copy in copies:
        copy.wait()


def swapped(array):
    return lax.ppermute(array, "head", [(0, 1), (1, 0)])


def across(array, first):
    count = lax.axis_size("section")
    edges = [(i, i + 1) for i in range(first, count - 1, 2)]
    return lax.ppermute(array, "section", edges + [(j, i) for i, j in edges])


def on_device(
    video_tokens,
    modulation,
    project_weight,
    output_weight,
    norm_gains,
    text_cache,
    text_count,
    video_keep,
    patch_order,
    stale_cache,
):
    sections = lax.axis_size("section")
    place = lax.axis_index("section").astype(jnp.int32).reshape(1)
    side = lax.axis_index("head").astype(jnp.int32).reshape(1)
    rows, model = video_tokens.shape
    size = norm_gains.shape[1]
    width = project_weight.shape[2]
    heads = width // size
    patch = stale_cache.shape[1]
    text_rows = text_cache.shape[1]
    keep = video_keep.reshape(-1, size)
    half_shape = jax.ShapeDtypeStruct((rows, model), bf16)
    side_shape = jax.ShapeDtypeStruct((patch, width), bf16)
    part_shape = jax.ShapeDtypeStruct((rows, width), bf16)
    total_shape = jax.ShapeDtypeStruct((patch, 2 * width), f32)
    stale_cache = in_hbm(stale_cache)

    normed, to_odd, to_even, values = pl.pallas_call(
        functools.partial(first_kernel, sections),
        out_shape=(half_shape, half_shape, half_shape, side_shape),
        in_specs=[SMEM, HBM, HBM, HBM, HBM],
        out_specs=(HBM,) * 4,
        scratch_shapes=[
            pltpu.SMEM(patch_order.shape, jnp.int32),
            pltpu.VMEM((rows, model), bf16),
            pltpu.VMEM(modulation.shape, f32),
            pltpu.VMEM((patch, width), bf16),
            pltpu.VMEM((patch, width), bf16),
            pltpu.VMEM((rows, model), bf16),
            pltpu.SemaphoreType.DMA((6,)),
            pltpu.SemaphoreType.DMA((8,)),
        ],
        compiler_params=params(10),
        cost_estimate=cost(10 * rows * model, 10 * rows * model),
        name="first",
    )(place, in_hbm(patch_order), in_hbm(video_tokens), in_hbm(modulation), stale_cache)

    odd_own = across(to_odd, 1)
    even_own = across(to_even, 0)
    even_values = across(values, 0)
    odd_values = across(values, 1)
    other = swapped(normed)

    weight_shape = jax.ShapeDtypeStruct((model, width), bf16)
    project_weight = in_hbm(project_weight)
    own_cache, own_keys, key_weight, value_weight = pl.pallas_call(
        own_rows_kernel,
        out_shape=(
            jax.ShapeDtypeStruct((2, rows, width), bf16),
            part_shape,
            weight_shape,
            weight_shape,
        ),
        in_specs=[VMEM, HBM, HBM],
        out_specs=(VMEM,) * 4,
        scratch_shapes=[
            pltpu.VMEM(norm_gains.shape, f32),
            pltpu.SemaphoreType.DMA((width // size,)),
            pltpu.SemaphoreType.DMA,
        ],
        compiler_params=params(10),
        cost_estimate=cost(4 * rows * model * width, 4 * rows * width),
        name="own_rows",
    )(normed, project_weight, in_hbm(norm_gains))

    fresh_cache, queries, keys, vbuf = pl.pallas_call(
        other_rows_kernel,
        out_shape=(
            jax.ShapeDtypeStruct((2, patch, width), bf16),
            side_shape,
            side_shape,
            jax.ShapeDtypeStruct((heads, patch, 2 * size), bf16),
        ),
        in_specs=[SMEM, SMEM, VMEM, HBM] + [VMEM] * 4 + [HBM, VMEM, VMEM],
        out_specs=(HBM,) + (VMEM,) * 3,
        scratch_shapes=[
            pltpu.VMEM((rows, model), bf16),
            pltpu.VMEM((2, rows, width), bf16),
            pltpu.VMEM((model, width), bf16),
            pltpu.SemaphoreType.DMA((12,)),
        ],
        compiler_params=params(16),
        cost_estimate=cost(8 * rows * model * width, 4 * rows * width),
        name="other_rows",
    )(
        place,
        side,
        normed,
        in_hbm(other),
        own_cache,
        own_keys,
        key_weight,
        value_weight,
        project_weight,
        norm_gains,
        keep,
    )

    odd_own, queries, keys = lax.optimization_barrier((odd_own, queries, keys))
    odd_other = swapped(odd_own)

    total = pl.pallas_call(
        own_kernel,
        out_shape=total_shape,
        in_specs=[SMEM, VMEM, VMEM, VMEM, HBM, VMEM],
        out_specs=VMEM,
        scratch_shapes=[
            pltpu.VMEM((2, text_rows, width), bf16),
            pltpu.VMEM((text_rows, width), bf16),
            pltpu.VMEM((heads, text_rows, 2 * size), bf16),
            pltpu.SemaphoreType.DMA,
        ],
        compiler_params=params(12),
        cost_estimate=cost(6 * patch * (patch + text_rows) * width, 6 * patch * width),
        name="own",
    )(text_count, queries, keys, vbuf, in_hbm(text_cache), norm_gains)

    even_own, total = lax.optimization_barrier((even_own, total))
    even_other = swapped(even_own)

    def near(edge, mine, other, total):
        buffers = []
        if edge == 0:
            mine = in_hbm(mine)
            buffers = [pltpu.VMEM((rows, model), bf16), pltpu.SemaphoreType.DMA((2,))]
        return pl.pallas_call(
            functools.partial(near_kernel, sections, edge),
            out_shape=(total_shape, jax.ShapeDtypeStruct((heads, patch, patch), bf16)),
            in_specs=[SMEM] * 3 + [VMEM if edge else HBM] + [VMEM] * 7,
            out_specs=(VMEM, VMEM),
            scratch_shapes=[
                pltpu.VMEM((patch, width), bf16),
                pltpu.VMEM((heads, patch, 2 * size), bf16),
            ]
            + buffers,
            input_output_aliases={10: 0},
            compiler_params=params(16),
            cost_estimate=cost(4 * patch * model * width, 6 * patch * width),
            name="near_even" if edge else "near_odd",
        )(
            place,
            side,
            patch_order,
            mine,
            other,
            key_weight,
            value_weight,
            norm_gains,
            queries,
            keep,
            total,
        )

    total, odd_weights = near(0, odd_own, odd_other, total)
    total, even_weights = near(1, even_own, even_other, total)

    def finish(flip):
        return pl.pallas_call(
            functools.partial(finish_kernel, sections, flip),
            out_shape=half_shape,
            in_specs=[SMEM] * 3 + [VMEM] * 7,
            out_specs=VMEM,
            scratch_shapes=[
                pltpu.VMEM((heads, patch, 2 * size), bf16),
                pltpu.VMEM((rows, 2 * width), f32),
                pltpu.VMEM((rows, width), bf16),
            ],
            compiler_params=params(20),
            cost_estimate=cost(2 * rows * width * model, 4 * rows * model),
            name="finish_sent" if flip else "finish_kept",
        )(
            place,
            side,
            patch_order,
            odd_weights,
            even_weights,
            odd_values,
            even_values,
            keep,
            total,
            output_weight,
        )

    sent = finish(True)
    received = swapped(sent)
    kept = finish(False)
    updated = pl.pallas_call(
        add_kernel,
        out_shape=half_shape,
        in_specs=[VMEM] * 4,
        out_specs=HBM,
        scratch_shapes=[pltpu.VMEM((rows, model), bf16), pltpu.SemaphoreType.DMA((4,))],
        compiler_params=params(8),
        cost_estimate=cost(6 * rows * model, 8 * rows * model),
        name="add",
    )(video_tokens, modulation, kept, received)
    return (updated, fresh_cache)


def solution(mesh):
    placed = (
        P(("groups", "section", "head"), None),
        P("groups", None),
        P(None, None, "head"),
        P("head", None),
        P(),
        P(None, "groups", "head"),
        P("groups"),
        P("groups"),
        P("groups"),
        P(None, ("groups", "section"), "head"),
    )

    return jax.shard_map(
        on_device,
        mesh=mesh,
        in_specs=placed,
        out_specs=(P(("groups", "section", "head"), None), P(None, ("groups", "section"), "head")),
        check_vma=False,
    )
```
